32 devices in a mesh: gx: 4 (over y, core), gy: 4 (over z), gz: 2 (over x).
Axes of the slice: x: 2, y: 2, z: 4, core: 2. Of those that a mesh axis runs over, the one named last changes fastest.
Arguments:
- positions: float32 [3, 4, 32, 2, 128], P(None, 'gx', ('gy', 'gz')), may hold values from 0 to 3
- velocities: float32 [3, 4, 32, 2, 128], P(None, 'gx', ('gy', 'gz')), may hold values from -6 to 6
- bead_keys: int32 [4, 32, 2, 128], P('gx', ('gy', 'gz')), may hold values from 0 to 1073741823
- counts: int32 [4, 32, 2], P('gx', ('gy', 'gz')), may hold values from 64 to 128
Outputs:
- half_kick: float32 [3, 4, 32, 2, 128], P(None, 'gx', 'gy', 'gz')
The draws below stay inside these ranges and needn't reach their ends.
Inputs may be any that keep to these rules, and one draw needn't show every extreme that they name: Slots from counts of a tile on are padding and take no part. `bead_keys`: the lowest bit of a key names the bead type, 0 water and 1 polymer.
All inputs are finite; a program needn't handle non-finite values.
Results may differ from the reference program's by a relative error of at most 0.0003.
Values sent between devices are 32-bit elements; how exact they have to be, the bound alone decides.
A program may use at most 64 MiB of HBM per device.

```python
import jax
import jax.numpy as jnp
from jax import lax

SLOTS = 128
SIDE = 3
NTX = 4
NTY = 32
NTZ = 2


def place_ends(values, own_key, smallest, top_value):
    index_at = [jax.random.randint(jax.random.fold_in(own_key, axis), (), 0, length) for axis, length in enumerate(values.shape)]
    main_axis = values.shape.index(max(values.shape))
    next_to = index_at[:main_axis] + [(index_at[main_axis] + 1) % values.shape[main_axis]] + index_at[main_axis + 1:]
    return values.at[tuple(index_at)].set(smallest).at[tuple(next_to)].set(top_value)


def levels(stream_key, shape, split, low, largest):
    def one(axis_at, blocks):
        heights = jax.random.uniform(jax.random.fold_in(jax.random.fold_in(stream_key, 6), axis_at), (blocks,), jnp.float32, low / len(split), largest / len(split))
        return jnp.repeat(jnp.exp(heights), shape[axis_at] // blocks).reshape((-1,) + (1,) * (len(shape) - axis_at - 1))

    factor_of = one(*split[0])
    for cut in split[1:]:
        factor_of = factor_of * one(*cut)
    return factor_of


def bell_draw(rng, extent, width, reach, split=(), kind=jnp.bfloat16):
    result = jax.random.normal(rng, extent, jnp.float32) * width
    if len(split) > 0:
        result = levels(rng, extent, split, -0.22, 0.18) * result
    return jnp.clip(result, min=-reach, max=reach).astype(kind)


def setup_inputs(seed: int = 0) -> dict:
    streams_of = jax.random.split(jax.random.key(seed), 5)
    return {
        "positions": jnp.clip(3.0 * jax.random.uniform(streams_of[0], (3, NTX, NTY, NTZ, SLOTS), jnp.float32) ** levels(streams_of[0], (3, NTX, NTY, NTZ, SLOTS), ((1, 4), (2, 8)), -0.2, 0.2), 0.0, 3.0),
        "velocities": bell_draw(streams_of[1], (3, NTX, NTY, NTZ, SLOTS), 1.0, 6.0, ((1, 4), (2, 8)), jnp.float32),
        "bead_keys": place_ends(jax.random.randint(streams_of[2], (NTX, NTY, NTZ, SLOTS), 0, 1073741824), jax.random.fold_in(streams_of[2], 1), 0, 1073741823).astype(jnp.int32),
        "counts": place_ends(jax.random.randint(streams_of[3], (NTX, NTY, NTZ), SLOTS // 2, SLOTS + 1), jax.random.fold_in(streams_of[3], 1), SLOTS // 2, SLOTS).astype(jnp.int32),
    }


soft_radius = 0.05
friction = 4.5
noise_amplitude = 15.0
like_repulsion = 25.0
unlike_extra = 15.0
kick_scale = 0.02
root_twelve = 3.4641016151377544

def pair_noise(first_keys, second_keys):
    hashed = (first_keys ^ second_keys) * 1103515245 + (first_keys + second_keys) * 12345
    hashed = hashed ^ hashed >> 15 & 131071
    hashed = hashed * 747796405
    hashed = hashed ^ hashed >> 13 & 524287
    fraction = (hashed >> 7 & 16777215).astype(jnp.float32) * (1.0 / 16777216.0)
    return root_twelve * (fraction - 0.5)

def pair_forces(own_motion, own_keys, other_motion, other_keys, other_counts, displace):
    slot_index = lax.broadcasted_iota(jnp.int32, other_keys.shape, 1)
    present = (slot_index < other_counts[:, None]).astype(jnp.float32)
    separation = [own_motion[component][:, :, None] - (other_motion[component][:, None, :] + displace[component]) for component in range(3)]
    squared = separation[0] * separation[0] + separation[1] * separation[1] + separation[2] * separation[2]
    distance = jnp.sqrt(squared)
    weight = jnp.maximum(1.0 - distance, 0.0) * present[:, None, :]
    inverse = 1.0 / jnp.maximum(distance, soft_radius)
    approach = separation[0] * (own_motion[3][:, :, None] - other_motion[3][:, None, :])
    approach = approach + separation[1] * (own_motion[4][:, :, None] - other_motion[4][:, None, :])
    approach = approach + separation[2] * (own_motion[5][:, :, None] - other_motion[5][:, None, :])
    approach = approach * inverse
    first_keys = own_keys[:, :, None]
    second_keys = other_keys[:, None, :]
    random_pair = pair_noise(first_keys, second_keys)
    repulsion = like_repulsion + unlike_extra * ((first_keys ^ second_keys) & 1).astype(jnp.float32)
    strength = (repulsion * weight - friction * weight * weight * approach + noise_amplitude * weight * random_pair) * inverse
    return jnp.stack([lax.optimization_barrier(jnp.sum(strength * part, axis=2)) for part in separation])

def reference(positions, velocities, bead_keys, counts):
    motion = jnp.concatenate([positions, velocities], axis=0)
    size_x, size_y, size_z, slots = bead_keys.shape
    plane = size_y * size_z
    own_motion = jnp.moveaxis(motion, 1, 0).reshape(size_x, 6, plane, slots)
    own_keys = bead_keys.reshape(size_x, plane, slots)
    summed = jnp.zeros((size_x, 3, plane, slots), jnp.float32)
    for off_x in range(3):
        for off_y in range(3):
            for off_z in range(3):
                moved = (1 - off_x, 1 - off_y, 1 - off_z)
                other_motion = jnp.moveaxis(jnp.roll(motion, moved, axis=(1, 2, 3)), 1, 0).reshape(size_x, 6, plane, slots)
                other_keys = jnp.roll(bead_keys, moved, axis=(0, 1, 2)).reshape(size_x, plane, slots)
                other_counts = jnp.roll(counts, moved, axis=(0, 1, 2)).reshape(size_x, plane)
                displace = jnp.array([SIDE * (off_x - 1), SIDE * (off_y - 1), SIDE * (off_z - 1)], jnp.float32)

                def one_plane(items, displace=displace):
                    return pair_forces(items[0], items[1], items[2], items[3], items[4], displace)
                summed = summed + lax.map(one_plane, (own_motion, own_keys, other_motion, other_keys, other_counts))
    slot_index = lax.broadcasted_iota(jnp.int32, bead_keys.shape, 3)
    occupied = (slot_index < counts[:, :, :, None]).astype(jnp.float32)
    force = jnp.moveaxis(summed, 1, 0).reshape(3, size_x, size_y, size_z, slots)
    return kick_scale * force * occupied[None]
```

```python
import functools

import jax
import jax.numpy as jnp
from jax import lax
from jax.experimental import pallas as pl
from jax.experimental.pallas import tpu as pltpu
from jax.sharding import PartitionSpec as P

SIDE = 3.0

soft_radius = 0.05
friction = 4.5
noise_amplitude = 15.0
like_repulsion = 25.0
unlike_extra = 15.0
kick_scale = 0.02
root_twelve = 3.4641016151377544

FAR = 1.0e9
ROWS = 8
GROUP = 128
MESH = pl.DeviceIdType.MESH


def gather_kernel(sizes, pos_in, vel_in, key_in, count_in, all_ref, pos_ref, vel_ref, key_ref, count_ref, packed, send, recv, edge_send, edge_recv, local, loads):
    nx, ny, nz, block_y, tiles_z = sizes
    gx, gy, gz = lax.axis_index("gx"), lax.axis_index("gy"), lax.axis_index("gz")
    slots = pos_ref.shape[-1]
    inputs = ((pos_in, pos_ref), (vel_in, vel_ref), (key_in, key_ref), (count_in, count_ref))
    fetches = [pltpu.make_async_copy(a, b, loads.at[k]) for k, (a, b) in enumerate(inputs)]
    for fetch in fetches:
        fetch.start()
    top = nz * block_y + 1
    barrier = pltpu.get_barrier_semaphore()

    def target(e, group, member):
        return (lax.rem(gx + e + nx, nx), lax.rem(gy + group + ny, ny), lax.rem(member + nz, nz))

    steps = (-1, 0, 1)
    for e in steps:
        for r in range(nz):
            if e or r:
                pl.semaphore_signal(barrier, inc=1, device_id=target(e, 0, gz + r), device_id_type=MESH)
        pl.semaphore_signal(barrier, inc=1, device_id=target(e, -1, nz - 1), device_id_type=MESH)
        pl.semaphore_signal(barrier, inc=1, device_id=target(e, 1, 0), device_id_type=MESH)

    for fetch in fetches:
        fetch.wait()
    lane = lax.broadcasted_iota(jnp.int32, (1, slots), 1)
    for y in range(block_y):
        for z in range(tiles_z):
            present = lane < count_ref[0, z, y]
            key = key_ref[0, y, pl.ds(z, 1), :]
            rows = [jnp.where(present, pos_ref[c, 0, y, pl.ds(z, 1), :], FAR) for c in range(3)]
            rows += [vel_ref[c, 0, y, pl.ds(z, 1), :] * friction for c in range(3)]
            rows += [(key >> 15).astype(jnp.float32), (key & 32767).astype(jnp.float32)]
            packed[y, z] = jnp.concatenate(rows, axis=0)

    def group_copy(e, r, slot_of):
        return pltpu.make_async_remote_copy(
            src_ref=packed,
            dst_ref=all_ref.at[1 - e, pl.ds(1 + slot_of * block_y, block_y)],
            send_sem=send.at[e + 1, r],
            recv_sem=recv.at[e + 1, r],
            device_id=target(e, 0, gz + r),
            device_id_type=MESH,
        )

    def edge_copy(e, side, member):
        first = side == 0
        return pltpu.make_async_remote_copy(
            src_ref=packed.at[pl.ds(0 if first else block_y - 1, 1)],
            dst_ref=all_ref.at[1 - e, pl.ds(top if first else 0, 1)],
            send_sem=edge_send.at[side, e + 1, member],
            recv_sem=edge_recv.at[side, e + 1],
            device_id=target(e, -1 if first else 1, member),
            device_id_type=MESH,
        )

    ends = jnp.where(gz == 0, 1, 0) + jnp.where(gz == nz - 1, 1, 0)
    pl.semaphore_wait(barrier, 3 * nz - 1 + 3 * nz * ends)

    for e in (-1, 1, 0):
        for r in range(nz):
            if e or r:
                group_copy(e, r, gz).start()

    def edges(side, act):
        for e in (-1, 1, 0):
            for member in range(nz):
                act(edge_copy(e, side, member))

    @pl.when(gz == 0)
    def _():
        edges(0, lambda c: c.start())

    @pl.when(gz == nz - 1)
    def _():
        edges(1, lambda c: c.start())

    mine = pltpu.make_async_copy(packed, all_ref.at[1, pl.ds(1 + gz * block_y, block_y)], local)
    mine.start()
    mine.wait()
    for e in steps:
        for r in range(nz):
            if e or r:
                copy = group_copy(e, r, lax.rem(gz - r + nz, nz))
                copy.wait_recv()
                copy.wait_send()
        for side in range(2):
            edge_copy(e, side, 0).wait_recv()

    @pl.when(gz == 0)
    def _():
        edges(0, lambda c: c.wait_send())

    @pl.when(gz == nz - 1)
    def _():
        edges(1, lambda c: c.wait_send())


def shell_of(tiles_z):
    layers = (0, None) if tiles_z == 2 else (-1, 0, 1)
    offsets = [(dx, dy, dz) for dx in (-1, 0, 1) for dy in (-1, 0, 1) for dz in layers]
    return [offset for offset in offsets if offset != (0, 0, 0)]


def pair_kernel(sizes, all_ref, out_ref, jbuf, column, forces, masks, places, sources, moved, limits):
    tiles_z, out_y, out_z = sizes
    slots = all_ref.shape[-1]
    tiles = out_y * out_z
    gz = lax.axis_index("gz")
    row = lax.broadcasted_iota(jnp.int32, (ROWS, slots), 0)
    lane = lax.broadcasted_iota(jnp.int32, (ROWS, slots), 1)
    low = jnp.where(row < 3, -1.0, -3.0e38)
    high = jnp.where(row < 3, SIDE + 1.0, 3.0e38)
    shell = shell_of(tiles_z)
    n = len(shell)
    padded_n = masks.shape[0] // tiles

    def candidate(k, y, z):
        dx, dy, dz = shell[k]
        if dz is None:
            v = all_ref[1 + dx, y + 1 + dy, 1 - z]
            shift_z = jnp.where(v < 0.5 * SIDE, SIDE, -SIDE)
        else:
            v = all_ref[1 + dx, y + 1 + dy, lax.rem(z + dz + tiles_z, tiles_z)]
            shift_z = SIDE * dz
        return v + jnp.where(
            row == 0, SIDE * dx, jnp.where(row == 1, SIDE * dy, jnp.where(row == 2, shift_z, 0.0))
        )

    def mark(tile, carry):
        y, z = tile // out_z, gz * out_z + tile % out_z
        rows = []
        for k in range(n):
            v = candidate(k, y, z)
            inside = jnp.where((v > low) & (v < high), 1.0, 0.0)
            rows.append(jnp.min(inside, axis=0, keepdims=True))
        rows += [jnp.zeros((1, slots), jnp.float32)] * (padded_n - n)
        masks[pl.ds(pl.multiple_of(tile * padded_n, 8), padded_n), :] = jnp.concatenate(rows, axis=0)
        return carry

    lax.fori_loop(0, tiles, mark, 0, unroll=2)

    def square(size, test):
        i = lax.broadcasted_iota(jnp.int32, (size, size), 0)
        j = lax.broadcasted_iota(jnp.int32, (size, size), 1)
        return jnp.where(test(i, j), 1.0, 0.0).astype(jnp.bfloat16)

    height = tiles * padded_n
    mask = masks[...]
    half = mask.astype(jnp.bfloat16)
    rank = jnp.dot(half, square(slots, lambda i, j: i < j), preferred_element_type=jnp.float32)
    inside = jnp.dot(half, jnp.ones((slots, slots), jnp.bfloat16), preferred_element_type=jnp.float32)
    start = jnp.concatenate(
        [
            jnp.dot(
                square(padded_n, lambda i, j: j < i),
                inside[t * padded_n : (t + 1) * padded_n].astype(jnp.bfloat16),
                preferred_element_type=jnp.float32,
            )
            for t in range(tiles)
        ],
        axis=0,
    ).astype(jnp.int32)
    inside = inside.astype(jnp.int32)
    lanes = lax.broadcasted_iota(jnp.int32, (height, slots), 1)
    left = jnp.where(mask > 0.5, lanes - rank.astype(jnp.int32), 0)
    lane_bits = (slots - 1).bit_length()
    for bit in range(lane_bits):
        near = pltpu.roll(left, slots - (1 << bit), 1)
        take = (near & (1 << bit)) != 0
        leaves = (left & (1 << bit)) != 0
        left = jnp.where(take, near, jnp.where(leaves, 0, left))
    source = lanes + left
    for bit in range(lane_bits):
        source = jnp.where((start & (1 << bit)) != 0, pltpu.roll(source, 1 << bit, 1), source)
    offset = (lanes - start) & (slots - 1)
    sources[...] = source & (slots - 1)
    places[...] = jnp.where(offset < inside, (start + offset) >> lane_bits, -1)
    ends = start + inside
    for t in range(tiles):
        last = t * padded_n + n - 1
        limits[0, t] = jnp.max(ends[last : last + 1])
        own_x = all_ref[1, 1 + t // out_z, gz * out_z + t % out_z, pl.ds(0, 1), :]
        limits[1, t] = jnp.sum(jnp.where(own_x < 0.5 * FAR, 1.0, 0.0)).astype(jnp.int32)

    def collect(tile, carry):
        y, z = tile // out_z, gz * out_z + tile % out_z
        first = tile * padded_n
        for k in range(n):
            index = jnp.broadcast_to(sources[pl.ds(first + k, 1), :], (ROWS, slots))
            moved[tile, k] = jnp.take_along_axis(candidate(k, y, z), index, axis=1, mode="promise_in_bounds")
        column[tile, :, :ROWS] = jnp.transpose(all_ref[1, y + 1, z])
        return carry

    lax.fori_loop(0, tiles, collect, 0, unroll=2)

    def one_tile(tile, carry):
        y, zz = tile // out_z, tile % out_z
        z = gz * out_z + zz
        own = all_ref[1, y + 1, z]
        first = tile * padded_n
        blocks = 1 + (limits[0, tile] + slots - 1) // slots
        count = limits[1, tile]
        jbuf[0] = own

        def fill(b, carry):
            block = jnp.full((ROWS, slots), FAR, jnp.float32)
            for k in range(n):
                block = jnp.where(places[pl.ds(first + k, 1), :] == b - 1, moved[tile, k], block)
            jbuf[b] = block
            return carry

        lax.fori_loop(1, blocks, fill, 0)
        groups = (count + GROUP - 1) // GROUP

        def one_group(g, carry):
            base = pl.multiple_of(g * GROUP, GROUP)

            def wide(c):
                return jnp.broadcast_to(column[tile, pl.ds(base, GROUP), c : c + 1], (GROUP, slots))

            xi = [wide(c) for c in range(6)]
            klo = wide(7).astype(jnp.int32)
            ki = wide(6).astype(jnp.int32) * 32768 + klo
            ai = ki * 12345
            ti = (klo & 1).astype(jnp.float32) * unlike_extra - 0.5 * unlike_extra

            def one_block(b, acc):
                def other(c):
                    return jbuf[b, pl.ds(c, 1), :]

                sep = [xi[c] - other(c) for c in range(3)]
                squared = sep[0] * sep[0] + sep[1] * sep[1] + sep[2] * sep[2]
                root = lax.rsqrt(jnp.maximum(squared, 1e-30))
                distance = squared * root
                inverse = jnp.minimum(root, 1.0 / soft_radius)
                weight = jnp.maximum(1.0 - distance, 0.0)
                dot = (
                    sep[0] * (xi[3] - other(3))
                    + sep[1] * (xi[4] - other(4))
                    + sep[2] * (xi[5] - other(5))
                )
                lo = other(7).astype(jnp.int32)
                kj = other(6).astype(jnp.int32) * 32768 + lo
                tj = 1.0 - 2.0 * (lo & 1).astype(jnp.float32)
                hashed = (ki ^ kj) * 1103515245 + (ai + kj * 12345)
                hashed = hashed ^ lax.shift_right_logical(hashed, 15)
                hashed = hashed * 747796405
                hashed = hashed ^ lax.shift_right_logical(hashed, 13)
                fraction = (lax.shift_right_logical(hashed, 7) & 16777215).astype(jnp.float32)
                unit = noise_amplitude * root_twelve
                push = (
                    fraction * (unit / 16777216.0)
                    + (like_repulsion + 0.5 * unlike_extra - 0.5 * unit)
                    + ti * tj
                )
                scaled = weight * inverse
                strength = scaled * (push - scaled * dot)
                return tuple(acc[c] + strength * sep[c] for c in range(3))

            zero = jnp.zeros((GROUP, slots), jnp.float32)
            acc = lax.fori_loop(0, blocks, one_block, (zero, zero, zero))
            for c in range(3):
                forces[tile, c, pl.ds(base, GROUP), :] = acc[c]
            return carry

        lax.fori_loop(0, groups, one_group, 0)
        return carry

    lax.fori_loop(0, tiles, one_tile, 0)

    def finish(tile, carry):
        lanes = lax.broadcasted_iota(jnp.int32, (slots, slots), 1)
        sums = [jnp.sum(forces[tile, c], axis=1, keepdims=True) for c in range(3)]
        turned = jnp.transpose(jnp.where(lanes == 0, sums[0], jnp.where(lanes == 1, sums[1], sums[2])))
        kick = jnp.where(lane[:3] < limits[1, tile], kick_scale * turned[:3], 0.0)
        for c in range(3):
            out_ref[c, 0, tile // out_z, pl.ds(tile % out_z, 1), :] = kick[c : c + 1]
        return carry

    lax.fori_loop(0, tiles, finish, 0, unroll=2)


def on_device(nx, ny, nz, positions, velocities, bead_keys, counts):
    _, _, block_y, tiles_z, slots = positions.shape
    out_y, out_z = block_y * nz, tiles_z // nz
    span = out_y + 2
    gathered = pl.pallas_call(
        functools.partial(gather_kernel, (nx, ny, nz, block_y, tiles_z)),
        out_shape=jax.ShapeDtypeStruct((3, span, tiles_z, ROWS, slots), jnp.float32),
        in_specs=[pl.BlockSpec(memory_space=pltpu.HBM)] * 4,
        out_specs=pl.BlockSpec(memory_space=pl.ANY),
        scratch_shapes=[
            pltpu.VMEM(positions.shape, jnp.float32),
            pltpu.VMEM(velocities.shape, jnp.float32),
            pltpu.VMEM(bead_keys.shape, jnp.int32),
            pltpu.SMEM((1, tiles_z, block_y), jnp.int32),
            pltpu.VMEM((block_y, tiles_z, ROWS, slots), jnp.float32),
            pltpu.SemaphoreType.DMA((3, nz)),
            pltpu.SemaphoreType.DMA((3, nz)),
            pltpu.SemaphoreType.DMA((2, 3, nz)),
            pltpu.SemaphoreType.DMA((2, 3)),
            pltpu.SemaphoreType.DMA,
            pltpu.SemaphoreType.DMA((4,)),
        ],
        compiler_params=pltpu.CompilerParams(
            collective_id=0, has_side_effects=True, vmem_limit_bytes=4194304
        ),
        name="gather_tiles",
    )(*(pltpu.with_memory_space_constraint(a, pltpu.HBM) for a in (positions, velocities, bead_keys, jnp.swapaxes(counts, 1, 2))))
    shells = len(shell_of(tiles_z))
    height = out_y * out_z * (-(-shells // 8) * 8)
    return pl.pallas_call(
        functools.partial(pair_kernel, (tiles_z, out_y, out_z)),
        out_shape=jax.ShapeDtypeStruct((3, 1, out_y, out_z, slots), jnp.float32),
        in_specs=[pl.BlockSpec(memory_space=pltpu.VMEM)],
        out_specs=pl.BlockSpec(memory_space=pltpu.VMEM),
        scratch_shapes=[
            pltpu.VMEM((1 + shells, ROWS, slots), jnp.float32),
            pltpu.VMEM((out_y * out_z, slots, slots), jnp.float32),
            pltpu.VMEM((out_y * out_z, 3, slots, slots), jnp.float32),
            pltpu.VMEM((height, slots), jnp.float32),
            pltpu.VMEM((height, slots), jnp.int32),
            pltpu.VMEM((height, slots), jnp.int32),
            pltpu.VMEM((out_y * out_z, shells, ROWS, slots), jnp.float32),
            pltpu.SMEM((2, out_y * out_z), jnp.int32),
        ],
        compiler_params=pltpu.CompilerParams(vmem_limit_bytes=16777216),
        name="pair_kicks",
    )(gathered)


def solution(mesh):
    in_specs = (
        P(None, "gx", ("gy", "gz"), None, None),
        P(None, "gx", ("gy", "gz"), None, None),
        P("gx", ("gy", "gz"), None, None),
        P("gx", ("gy", "gz"), None),
    )
    out_specs = P(None, "gx", "gy", "gz", None)
    nx, ny, nz = mesh.shape["gx"], mesh.shape["gy"], mesh.shape["gz"]
    return jax.shard_map(
        functools.partial(on_device, nx, ny, nz),
        mesh=mesh,
        in_specs=in_specs,
        out_specs=out_specs,
        check_vma=False,
    )
```

```python
import functools

import jax
import jax.numpy as jnp
from jax import lax
from jax.experimental import pallas as pl
from jax.experimental.pallas import tpu as pltpu
from jax.sharding import PartitionSpec as P

SIDE = 3.0

soft_radius = 0.05
friction = 4.5
noise_amplitude = 15.0
like_repulsion = 25.0
unlike_extra = 15.0
kick_scale = 0.02
root_twelve = 3.4641016151377544

FAR = 1.0e9
ROWS = 8
KEY_A = 1103515245
KEY_B = 12345
KEY_C = 747796405
STEP = 16
UNIT = noise_amplitude * root_twelve / 2147483648.0
MESH = pl.DeviceIdType.MESH


def gather_kernel(sizes, pos_in, vel_in, key_in, count_in, all_ref, pos_ref, vel_ref, key_ref, count_ref, packed, send, recv, edge_send, edge_recv, local, loads):
    nx, ny, nz, block_y, tiles_z = sizes
    gx, gy, gz = lax.axis_index("gx"), lax.axis_index("gy"), lax.axis_index("gz")
    slots = pos_ref.shape[-1]
    inputs = ((pos_in, pos_ref), (vel_in, vel_ref), (key_in, key_ref), (count_in, count_ref))
    fetches = [pltpu.make_async_copy(a, b, loads.at[k]) for k, (a, b) in enumerate(inputs)]
    for fetch in fetches:
        fetch.start()
    top = nz * block_y + 1
    barrier = pltpu.get_barrier_semaphore()

    def target(e, group, member):
        return (lax.rem(gx + e + nx, nx), lax.rem(gy + group + ny, ny), lax.rem(member + nz, nz))

    steps = (-1, 0, 1)
    for e in steps:
        for r in range(nz):
            if e or r:
                pl.semaphore_signal(barrier, inc=1, device_id=target(e, 0, gz + r), device_id_type=MESH)
        pl.semaphore_signal(barrier, inc=1, device_id=target(e, -1, nz - 1), device_id_type=MESH)
        pl.semaphore_signal(barrier, inc=1, device_id=target(e, 1, 0), device_id_type=MESH)

    for fetch in fetches:
        fetch.wait()
    lane = lax.broadcasted_iota(jnp.int32, (1, slots), 1)
    for y in range(block_y):
        for z in range(tiles_z):
            present = lane < count_ref[0, z, y]
            key = key_ref[0, y, pl.ds(z, 1), :]
            rows = [jnp.where(present, pos_ref[c, 0, y, pl.ds(z, 1), :], FAR) for c in range(3)]
            rows += [vel_ref[c, 0, y, pl.ds(z, 1), :] * (friction / UNIT) for c in range(3)]
            rows += [(key >> 15).astype(jnp.float32), (key & 32767).astype(jnp.float32)]
            packed[y, z] = jnp.concatenate(rows, axis=0)

    def group_copy(e, r, slot_of):
        return pltpu.make_async_remote_copy(
            src_ref=packed,
            dst_ref=all_ref.at[1 - e, pl.ds(1 + slot_of * block_y, block_y)],
            send_sem=send.at[e + 1, r],
            recv_sem=recv.at[e + 1, r],
            device_id=target(e, 0, gz + r),
            device_id_type=MESH,
        )

    def edge_copy(e, side, member):
        first = side == 0
        return pltpu.make_async_remote_copy(
            src_ref=packed.at[pl.ds(0 if first else block_y - 1, 1)],
            dst_ref=all_ref.at[1 - e, pl.ds(top if first else 0, 1)],
            send_sem=edge_send.at[side, e + 1, member],
            recv_sem=edge_recv.at[side, e + 1],
            device_id=target(e, -1 if first else 1, member),
            device_id_type=MESH,
        )

    ends = jnp.where(gz == 0, 1, 0) + jnp.where(gz == nz - 1, 1, 0)
    pl.semaphore_wait(barrier, 3 * nz - 1 + 3 * nz * ends)

    for e in (-1, 1, 0):
        for r in range(nz):
            if e or r:
                group_copy(e, r, gz).start()

    def edges(side, act):
        for e in (-1, 1, 0):
            for member in range(nz):
                act(edge_copy(e, side, member))

    @pl.when(gz == 0)
    def _():
        edges(0, lambda c: c.start())

    @pl.when(gz == nz - 1)
    def _():
        edges(1, lambda c: c.start())

    mine = pltpu.make_async_copy(packed, all_ref.at[1, pl.ds(1 + gz * block_y, block_y)], local)
    mine.start()
    mine.wait()
    for e in steps:
        for r in range(nz):
            if e or r:
                copy = group_copy(e, r, lax.rem(gz - r + nz, nz))
                copy.wait_recv()
                copy.wait_send()
        for side in range(2):
            edge_copy(e, side, 0).wait_recv()

    @pl.when(gz == 0)
    def _():
        edges(0, lambda c: c.wait_send())

    @pl.when(gz == nz - 1)
    def _():
        edges(1, lambda c: c.wait_send())


def shell_of(tiles_z):
    layers = (0, None) if tiles_z == 2 else (-1, 0, 1)
    offsets = [(dx, dy, dz) for dx in (-1, 0, 1) for dy in (-1, 0, 1) for dz in layers]
    return [offset for offset in offsets if offset != (0, 0, 0)]


def pair_kernel(sizes, all_ref, out_ref, masks, places, moved, moved_keys, near, near_keys, wide, wide_keys, forces, limits):
    tiles_z, out_y, out_z = sizes
    slots = all_ref.shape[-1]
    span = all_ref.shape[1]
    gz = lax.axis_index("gz")
    shell = shell_of(tiles_z)
    n = len(shell)
    lane_bits = (slots - 1).bit_length()
    quarter = slots // 4
    flat = all_ref.reshape(3 * span * tiles_z * ROWS, slots)
    lane = lax.broadcasted_iota(jnp.int32, (out_y, slots), 1)

    def rows(dx, dy, z, c):
        start = (((1 + dx) * span + 1 + dy) * tiles_z + z) * ROWS + c
        return flat[pl.ds(start, out_y, stride=tiles_z * ROWS), :]

    def keys_of(dx, dy, z):
        return rows(dx, dy, z, 6).astype(jnp.int32) * 32768 + rows(dx, dy, z, 7).astype(jnp.int32)

    def spread(zz, z):
        def one(y, carry):
            tile = zz * out_y + y
            column = jnp.transpose(all_ref[1, y + 1, z])
            for c in range(6):
                wide[tile, c] = jnp.broadcast_to(column[:, c : c + 1], (slots, slots))
            low = jnp.broadcast_to(column[:, 7:8], (slots, slots)).astype(jnp.int32)
            key = jnp.broadcast_to(column[:, 6:7], (slots, slots)).astype(jnp.int32) * 32768 + low
            wide_keys[tile, 0] = key
            wide_keys[tile, 1] = key * KEY_B
            kind = (low & 1).astype(jnp.float32) * (unlike_extra / UNIT)
            level = (like_repulsion - 0.5 * noise_amplitude * root_twelve) / UNIT
            wide[tile, 6] = level + kind
            wide[tile, 7] = (level + unlike_extra / UNIT) - kind
            return carry

        lax.fori_loop(0, out_y, one, 0)

    def place_candidates(z):
        def position(k):
            dx, dy, dz = shell[k]
            other = 1 - z if dz is None else lax.rem(z + dz + tiles_z, tiles_z)
            p = [rows(dx, dy, other, c) for c in range(3)]
            if dx:
                p[0] = p[0] + SIDE * dx
            if dy:
                p[1] = p[1] + SIDE * dy
            if dz is None:
                p[2] = p[2] + jnp.where(p[2] < 0.5 * SIDE, SIDE, -SIDE)
            elif dz:
                p[2] = p[2] + SIDE * dz
            return p, other

        for k in range(n):
            p, _ = position(k)
            inside = None
            for c in range(3):
                if shell[k][c] != 0:
                    test = (p[c] > -1.0) & (p[c] < SIDE + 1.0)
                    inside = test if inside is None else inside & test
            masks[pl.ds(k * out_y, out_y), :] = jnp.where(inside, 1.0, 0.0)

        i = lax.broadcasted_iota(jnp.int32, (slots, 5 * slots), 0)
        j = lax.broadcasted_iota(jnp.int32, (slots, 5 * slots), 1)
        limit = jnp.where(j < slots, j + 1, (j >> lane_bits) * quarter)
        below = jnp.where(i < limit, 1.0, 0.0).astype(jnp.bfloat16)
        sums = jnp.dot(masks[...].astype(jnp.bfloat16), below, preferred_element_type=jnp.float32)
        start = jnp.zeros((out_y, slots), jnp.float32)
        for k in range(n):
            part = [sums[k * out_y : (k + 1) * out_y, q * slots : (q + 1) * slots] for q in range(5)]
            first = start.astype(jnp.int32)
            want = (lane - first) & (slots - 1)
            level = want.astype(jnp.float32)
            at = jnp.where(
                part[2] <= level,
                jnp.where(part[3] <= level, 3 * quarter, 2 * quarter),
                jnp.where(part[1] <= level, quarter, 0),
            )
            bit = quarter // 2
            while bit:
                seen = jnp.take_along_axis(part[0], at + (bit - 1), axis=1, mode="promise_in_bounds")
                at = jnp.where(seen <= level, at + bit, at)
                bit //= 2
            places[k] = jnp.where(level < part[4], (first + want) >> lane_bits, -1)
            start = start + part[4]
            p, other = position(k)
            dx, dy, _ = shell[k]
            p += [rows(dx, dy, other, c) for c in range(3, 6)]
            for c in range(6):
                moved[k, c] = jnp.take_along_axis(p[c], at, axis=1, mode="promise_in_bounds")
            moved_keys[k] = jnp.take_along_axis(keys_of(dx, dy, other), at, axis=1, mode="promise_in_bounds")
        return start

    def keep(block, motion, key):
        for c in range(6):
            near[block, c] = motion[c]
        near[block, 6] = (key & 1).astype(jnp.float32)
        near_keys[block, 0] = key
        near_keys[block, 1] = key * KEY_B

    def assemble(block, carry):
        motion = [jnp.full((out_y, slots), FAR if c < 3 else 0.0, jnp.float32) for c in range(6)]
        key = jnp.zeros((out_y, slots), jnp.int32)
        for k in range(n):
            here = places[k] == block - 1
            motion = [jnp.where(here, moved[k, c], motion[c]) for c in range(6)]
            key = jnp.where(here, moved_keys[k], key)
        keep(block, motion, key)
        return carry

    def pair_block(tile, y, block, height, fresh):
        other = [jnp.broadcast_to(near[block, c, pl.ds(y, 1), :], (8, slots)) for c in range(7)]
        kj = jnp.broadcast_to(near_keys[block, 0, pl.ds(y, 1), :], (8, slots))
        bj = jnp.broadcast_to(near_keys[block, 1, pl.ds(y, 1), :], (8, slots))
        even = other[6] < 0.5
        for g in range(0, height, 8):
            at = pl.ds(g, 8)
            sep = [wide[tile, c, at, :] - other[c] for c in range(3)]
            squared = sep[0] * sep[0] + sep[1] * sep[1] + sep[2] * sep[2]
            root = lax.rsqrt(jnp.maximum(squared, 1e-30))
            scaled = jnp.maximum(1.0 - squared * root, 0.0) * jnp.minimum(root, 1.0 / soft_radius)
            dot = sep[0] * (wide[tile, 3, at, :] - other[3])
            dot = dot + sep[1] * (wide[tile, 4, at, :] - other[4])
            dot = dot + sep[2] * (wide[tile, 5, at, :] - other[5])
            hashed = (wide_keys[tile, 0, at, :] ^ kj) * KEY_A + (wide_keys[tile, 1, at, :] + bj)
            hashed = hashed ^ lax.shift_right_logical(hashed, 15)
            hashed = hashed * KEY_C
            hashed = hashed ^ lax.shift_right_logical(hashed, 13)
            push = (hashed & 0x7FFFFF80).astype(jnp.float32)
            push = push + jnp.where(even, wide[tile, 6, at, :], wide[tile, 7, at, :])
            strength = scaled * (push - scaled * dot)
            for c in range(3):
                term = strength * sep[c]
                forces[tile, c, at, :] = term if fresh else forces[tile, c, at, :] + term

    def tile_pairs(tile, carry):
        y = tile % out_y
        blocks = limits[0, tile]
        heights = list(range(slots // 2, slots + 1, STEP))

        def at_height(height):
            def run():
                pair_block(tile, y, 0, height, True)

                def one(block, carry):
                    pair_block(tile, y, block, height, False)
                    return carry

                lax.fori_loop(1, blocks, one, 0)

            return run

        which = jnp.clip((limits[1, tile] + STEP - 1) // STEP - heights[0] // STEP, 0, len(heights) - 1)
        lax.switch(which, [at_height(h) for h in heights])
        return carry

    ones = jnp.ones((8, slots), jnp.bfloat16)
    for zz in range(out_z):
        z = gz * out_z + zz
        spread(zz, z)
        total = place_candidates(z)
        own = [rows(0, 0, z, c) for c in range(6)]
        present = own[0] < 0.5 * FAR
        keep(0, own, keys_of(0, 0, z))
        blocks = 1 + ((total.astype(jnp.int32) + (slots - 1)) >> lane_bits)
        count = jnp.sum(jnp.where(present, 1.0, 0.0), axis=1, keepdims=True).astype(jnp.int32)
        for y in range(out_y):
            limits[0, zz * out_y + y] = blocks[y, 0]
            limits[1, zz * out_y + y] = count[y, 0]
        lax.fori_loop(1, jnp.max(blocks), assemble, 0)
        lax.fori_loop(zz * out_y, (zz + 1) * out_y, tile_pairs, 0)
        for y in range(out_y):
            tile = zz * out_y + y
            for c in range(3):
                whole = forces[tile, c]
                high = whole.astype(jnp.bfloat16)
                low = (whole - high.astype(jnp.float32)).astype(jnp.bfloat16)
                kick = sum(
                    lax.dot_general(ones, part, (((1,), (1,)), ((), ())), preferred_element_type=jnp.float32)
                    for part in (high, low)
                )
                out_ref[c, 0, y, pl.ds(zz, 1), :] = jnp.where(present[y : y + 1], kick_scale * UNIT * kick[:1], 0.0)


def on_device(nx, ny, nz, positions, velocities, bead_keys, counts):
    _, _, block_y, tiles_z, slots = positions.shape
    out_y, out_z = block_y * nz, tiles_z // nz
    span = out_y + 2
    gathered = pl.pallas_call(
        functools.partial(gather_kernel, (nx, ny, nz, block_y, tiles_z)),
        out_shape=jax.ShapeDtypeStruct((3, span, tiles_z, ROWS, slots), jnp.float32),
        in_specs=[pl.BlockSpec(memory_space=pltpu.HBM)] * 4,
        out_specs=pl.BlockSpec(memory_space=pl.ANY),
        scratch_shapes=[
            pltpu.VMEM(positions.shape, jnp.float32),
            pltpu.VMEM(velocities.shape, jnp.float32),
            pltpu.VMEM(bead_keys.shape, jnp.int32),
            pltpu.SMEM((1, tiles_z, block_y), jnp.int32),
            pltpu.VMEM((block_y, tiles_z, ROWS, slots), jnp.float32),
            pltpu.SemaphoreType.DMA((3, nz)),
            pltpu.SemaphoreType.DMA((3, nz)),
            pltpu.SemaphoreType.DMA((2, 3, nz)),
            pltpu.SemaphoreType.DMA((2, 3)),
            pltpu.SemaphoreType.DMA,
            pltpu.SemaphoreType.DMA((4,)),
        ],
        compiler_params=pltpu.CompilerParams(
            collective_id=0, has_side_effects=True, vmem_limit_bytes=4194304
        ),
        name="gather_tiles",
    )(*(pltpu.with_memory_space_constraint(a, pltpu.HBM) for a in (positions, velocities, bead_keys, jnp.swapaxes(counts, 1, 2))))
    shells = len(shell_of(tiles_z))
    tiles = out_y * out_z
    return pl.pallas_call(
        functools.partial(pair_kernel, (tiles_z, out_y, out_z)),
        out_shape=jax.ShapeDtypeStruct((3, 1, out_y, out_z, slots), jnp.float32),
        in_specs=[pl.BlockSpec(memory_space=pltpu.VMEM)],
        out_specs=pl.BlockSpec(memory_space=pltpu.VMEM),
        scratch_shapes=[
            pltpu.VMEM((shells * out_y, slots), jnp.float32),
            pltpu.VMEM((shells, out_y, slots), jnp.int32),
            pltpu.VMEM((shells, 6, out_y, slots), jnp.float32),
            pltpu.VMEM((shells, out_y, slots), jnp.int32),
            pltpu.VMEM((1 + shells, 7, out_y, slots), jnp.float32),
            pltpu.VMEM((1 + shells, 2, out_y, slots), jnp.int32),
            pltpu.VMEM((tiles, 8, slots, slots), jnp.float32),
            pltpu.VMEM((tiles, 2, slots, slots), jnp.int32),
            pltpu.VMEM((tiles, 3, slots, slots), jnp.float32),
            pltpu.SMEM((2, tiles), jnp.int32),
        ],
        compiler_params=pltpu.CompilerParams(vmem_limit_bytes=25165824),
        name="pair_kicks",
    )(gathered)


def solution(mesh):
    in_specs = (
        P(None, "gx", ("gy", "gz"), None, None),
        P(None, "gx", ("gy", "gz"), None, None),
        P("gx", ("gy", "gz"), None, None),
        P("gx", ("gy", "gz"), None),
    )
    out_specs = P(None, "gx", "gy", "gz", None)
    nx, ny, nz = mesh.shape["gx"], mesh.shape["gy"], mesh.shape["gz"]
    return jax.shard_map(
        functools.partial(on_device, nx, ny, nz),
        mesh=mesh,
        in_specs=in_specs,
        out_specs=out_specs,
        check_vma=False,
    )
```

```python
import functools

import jax
import jax.numpy as jnp
from jax import lax
from jax.experimental import pallas as pl
from jax.experimental.pallas import tpu as pltpu
from jax.sharding import PartitionSpec as P

SIDE = 3.0

soft_radius = 0.05
friction = 4.5
noise_amplitude = 15.0
like_repulsion = 25.0
unlike_extra = 15.0
kick_scale = 0.02
root_twelve = 3.4641016151377544

FAR = 1.0e9
ROWS = 8
KEY_A = 1103515245
KEY_B = 12345
KEY_C = 747796405
STEP = 16
UNIT = noise_amplitude * root_twelve / 2147483648.0
MESH = pl.DeviceIdType.MESH


def pair_strength(own, own_key, own_offset, own_even, own_odd, other, key, offset, even):
    sep = [own[c] - other[c] for c in range(3)]
    squared = sep[0] * sep[0] + sep[1] * sep[1] + sep[2] * sep[2]
    root = lax.rsqrt(jnp.maximum(squared, 1e-30))
    scaled = jnp.maximum(1.0 - squared * root, 0.0) * jnp.minimum(root, 1.0 / soft_radius)
    dot = sep[0] * (own[3] - other[3]) + sep[1] * (own[4] - other[4]) + sep[2] * (own[5] - other[5])
    hashed = (own_key ^ key) * KEY_A + (own_offset + offset)
    hashed = hashed ^ lax.shift_right_logical(hashed, 15)
    hashed = hashed * KEY_C
    hashed = hashed ^ lax.shift_right_logical(hashed, 13)
    push = (hashed & 0x7FFFFF80).astype(jnp.float32) + jnp.where(even, own_even, own_odd)
    strength = scaled * (push - scaled * dot)
    return [strength * part for part in sep]


def own_tile(tile, rows, select, wide, wide_keys, forces):
    slots = rows.shape[1]
    high = rows.astype(jnp.bfloat16).astype(jnp.float32)
    middle = (rows - high).astype(jnp.bfloat16).astype(jnp.float32)
    column = jnp.transpose(jnp.concatenate([high, middle, rows - high - middle], axis=0)).astype(jnp.bfloat16)
    spread = jnp.dot(column, select[...], preferred_element_type=jnp.float32)
    key_row = rows[6:7].astype(jnp.int32) * 32768 + rows[7:8].astype(jnp.int32)
    other = [jnp.broadcast_to(rows[c : c + 1], (8, slots)) for c in range(6)]
    key = jnp.broadcast_to(key_row, (8, slots))
    offset = key * KEY_B
    even = (key & 1) == 0
    level = (like_repulsion - 0.5 * noise_amplitude * root_twelve) / UNIT
    for g in range(0, slots, 8):
        at = pl.ds(g, 8)
        part = [spread[g : g + 8, c * slots : (c + 1) * slots] for c in range(8)]
        low = part[7].astype(jnp.int32)
        own_key = part[6].astype(jnp.int32) * 32768 + low
        own_offset = own_key * KEY_B
        kind = (low & 1).astype(jnp.float32) * (unlike_extra / UNIT)
        own_even = level + kind
        own_odd = (level + unlike_extra / UNIT) - kind
        for c in range(6):
            wide[tile, c, at, :] = part[c]
        wide[tile, 6, at, :] = own_even
        wide[tile, 7, at, :] = own_odd
        wide_keys[tile, 0, at, :] = own_key
        wide_keys[tile, 1, at, :] = own_offset
        terms = pair_strength(part, own_key, own_offset, own_even, own_odd, other, key, offset, even)
        for c in range(3):
            forces[tile, c, at, :] = terms[c]


def gather_kernel(sizes, pos_in, vel_in, key_in, count_in, all_ref, wide, wide_keys, forces, pos_ref, vel_ref, key_ref, count_ref, packed, select, send, recv, edge_send, edge_recv, local, loads):
    nx, ny, nz, block_y, tiles_z = sizes
    gx, gy, gz = lax.axis_index("gx"), lax.axis_index("gy"), lax.axis_index("gz")
    slots = pos_ref.shape[-1]
    inputs = ((pos_in, pos_ref), (vel_in, vel_ref), (key_in, key_ref), (count_in, count_ref))
    fetches = [pltpu.make_async_copy(a, b, loads.at[k]) for k, (a, b) in enumerate(inputs)]
    for fetch in fetches:
        fetch.start()
    top = nz * block_y + 1
    barrier = pltpu.get_barrier_semaphore()

    def target(e, group, member):
        return (lax.rem(gx + e + nx, nx), lax.rem(gy + group + ny, ny), lax.rem(member + nz, nz))

    steps = (-1, 0, 1)
    for e in steps:
        for r in range(nz):
            if e or r:
                pl.semaphore_signal(barrier, inc=1, device_id=target(e, 0, gz + r), device_id_type=MESH)
        pl.semaphore_signal(barrier, inc=1, device_id=target(e, -1, nz - 1), device_id_type=MESH)
        pl.semaphore_signal(barrier, inc=1, device_id=target(e, 1, 0), device_id_type=MESH)

    row = lax.broadcasted_iota(jnp.int32, select.shape, 0)
    column = lax.broadcasted_iota(jnp.int32, select.shape, 1)
    chosen = (row & (ROWS - 1)) == (column >> (slots - 1).bit_length())
    select[...] = jnp.where(chosen, 1.0, 0.0).astype(jnp.bfloat16)
    for fetch in fetches:
        fetch.wait()
    lane = lax.broadcasted_iota(jnp.int32, (1, slots), 1)
    for y in range(block_y):
        for z in range(tiles_z):
            present = lane < count_ref[0, z, y]
            key = key_ref[0, y, pl.ds(z, 1), :]
            rows = [jnp.where(present, pos_ref[c, 0, y, pl.ds(z, 1), :], FAR) for c in range(3)]
            rows += [vel_ref[c, 0, y, pl.ds(z, 1), :] * (friction / UNIT) for c in range(3)]
            rows += [(key >> 15).astype(jnp.float32), (key & 32767).astype(jnp.float32)]
            packed[y, z] = jnp.concatenate(rows, axis=0)

    def group_copy(e, r, slot_of):
        return pltpu.make_async_remote_copy(
            src_ref=packed,
            dst_ref=all_ref.at[1 - e, pl.ds(1 + slot_of * block_y, block_y)],
            send_sem=send.at[e + 1, r],
            recv_sem=recv.at[e + 1, r],
            device_id=target(e, 0, gz + r),
            device_id_type=MESH,
        )

    def edge_copy(e, side, member):
        first = side == 0
        return pltpu.make_async_remote_copy(
            src_ref=packed.at[pl.ds(0 if first else block_y - 1, 1)],
            dst_ref=all_ref.at[1 - e, pl.ds(top if first else 0, 1)],
            send_sem=edge_send.at[side, e + 1, member],
            recv_sem=edge_recv.at[side, e + 1],
            device_id=target(e, -1 if first else 1, member),
            device_id_type=MESH,
        )

    ends = jnp.where(gz == 0, 1, 0) + jnp.where(gz == nz - 1, 1, 0)
    pl.semaphore_wait(barrier, 3 * nz - 1 + 3 * nz * ends)

    def edges(side, act):
        for e in (-1, 1, 0):
            for member in range(nz):
                act(edge_copy(e, side, member))

    @pl.when(gz == 0)
    def _():
        edges(0, lambda c: c.start())

    @pl.when(gz == nz - 1)
    def _():
        edges(1, lambda c: c.start())

    for r in reversed(range(nz)):
        for e in (0, -1, 1):
            if e or r:
                group_copy(e, r, gz).start()

    mine = pltpu.make_async_copy(packed, all_ref.at[1, pl.ds(1 + gz * block_y, block_y)], local)
    mine.start()
    out_y, out_z = nz * block_y, tiles_z // nz
    for zz in range(out_z):

        def local(y, carry, zz=zz):
            own_tile(zz * out_y + gz * block_y + y, packed[y, gz * out_z + zz], select, wide, wide_keys, forces)
            return carry

        lax.fori_loop(0, block_y, local, 0)

    for r in range(1, nz):
        slot_of = lax.rem(gz - r + nz, nz)
        group_copy(0, r, slot_of).wait_recv()
        for zz in range(out_z):

            def remote(y, carry, zz=zz, slot_of=slot_of):
                at = slot_of * block_y + y
                own_tile(zz * out_y + at, all_ref[1, 1 + at, gz * out_z + zz], select, wide, wide_keys, forces)
                return carry

            lax.fori_loop(0, block_y, remote, 0)

    mine.wait()
    for e in steps:
        for r in range(nz):
            if e or r:
                copy = group_copy(e, r, lax.rem(gz - r + nz, nz))
                if e:
                    copy.wait_recv()
                copy.wait_send()
        for side in range(2):
            edge_copy(e, side, 0).wait_recv()

    @pl.when(gz == 0)
    def _():
        edges(0, lambda c: c.wait_send())

    @pl.when(gz == nz - 1)
    def _():
        edges(1, lambda c: c.wait_send())


def shell_of(tiles_z):
    layers = (0, None) if tiles_z == 2 else (-1, 0, 1)
    offsets = [(dx, dy, dz) for dx in (-1, 0, 1) for dy in (-1, 0, 1) for dz in layers]
    return [offset for offset in offsets if offset != (0, 0, 0)]


def pair_kernel(sizes, all_ref, wide, wide_keys, own_forces, out_ref, masks, places, moved, moved_keys, near, near_keys, forces, limits):
    tiles_z, out_y, out_z = sizes
    slots = all_ref.shape[-1]
    span = all_ref.shape[1]
    gz = lax.axis_index("gz")
    shell = shell_of(tiles_z)
    n = len(shell)
    lane_bits = (slots - 1).bit_length()
    quarter = slots // 4
    flat = all_ref.reshape(3 * span * tiles_z * ROWS, slots)
    lane = lax.broadcasted_iota(jnp.int32, (out_y, slots), 1)

    def rows(dx, dy, z, c):
        start = (((1 + dx) * span + 1 + dy) * tiles_z + z) * ROWS + c
        return flat[pl.ds(start, out_y, stride=tiles_z * ROWS), :]

    def keys_of(dx, dy, z):
        return rows(dx, dy, z, 6).astype(jnp.int32) * 32768 + rows(dx, dy, z, 7).astype(jnp.int32)

    def place_candidates(z):
        def position(k):
            dx, dy, dz = shell[k]
            other = 1 - z if dz is None else lax.rem(z + dz + tiles_z, tiles_z)
            p = [rows(dx, dy, other, c) for c in range(3)]
            if dx:
                p[0] = p[0] + SIDE * dx
            if dy:
                p[1] = p[1] + SIDE * dy
            if dz is None:
                p[2] = p[2] + jnp.where(p[2] < 0.5 * SIDE, SIDE, -SIDE)
            elif dz:
                p[2] = p[2] + SIDE * dz
            return p, other

        for k in range(n):
            p, _ = position(k)
            inside = None
            for c in range(3):
                if shell[k][c] != 0:
                    test = (p[c] > -1.0) & (p[c] < SIDE + 1.0)
                    inside = test if inside is None else inside & test
            masks[pl.ds(k * out_y, out_y), :] = jnp.where(inside, 1.0, 0.0)

        i = lax.broadcasted_iota(jnp.int32, (slots, 5 * slots), 0)
        j = lax.broadcasted_iota(jnp.int32, (slots, 5 * slots), 1)
        limit = jnp.where(j < slots, j + 1, (j >> lane_bits) * quarter)
        below = jnp.where(i < limit, 1.0, 0.0).astype(jnp.bfloat16)
        sums = jnp.dot(masks[...].astype(jnp.bfloat16), below, preferred_element_type=jnp.float32)
        start = jnp.zeros((out_y, slots), jnp.float32)
        for k in range(n):
            part = [sums[k * out_y : (k + 1) * out_y, q * slots : (q + 1) * slots] for q in range(5)]
            first = start.astype(jnp.int32)
            want = (lane - first) & (slots - 1)
            level = want.astype(jnp.float32)
            at = jnp.where(
                part[2] <= level,
                jnp.where(part[3] <= level, 3 * quarter, 2 * quarter),
                jnp.where(part[1] <= level, quarter, 0),
            )
            bit = quarter // 2
            while bit:
                seen = jnp.take_along_axis(part[0], at + (bit - 1), axis=1, mode="promise_in_bounds")
                at = jnp.where(seen <= level, at + bit, at)
                bit //= 2
            places[k] = jnp.where(level < part[4], (first + want) >> lane_bits, -1)
            start = start + part[4]
            p, other = position(k)
            dx, dy, _ = shell[k]
            p += [rows(dx, dy, other, c) for c in range(3, 6)]
            for c in range(6):
                moved[k, c] = jnp.take_along_axis(p[c], at, axis=1, mode="promise_in_bounds")
            moved_keys[k] = jnp.take_along_axis(keys_of(dx, dy, other), at, axis=1, mode="promise_in_bounds")
        return start

    def keep(block, motion, key):
        for c in range(6):
            near[block, c] = motion[c]
        near[block, 6] = (key & 1).astype(jnp.float32)
        near_keys[block, 0] = key
        near_keys[block, 1] = key * KEY_B

    def assemble(block, carry):
        motion = [jnp.full((out_y, slots), FAR if c < 3 else 0.0, jnp.float32) for c in range(6)]
        key = jnp.zeros((out_y, slots), jnp.int32)
        for k in range(n):
            here = places[k] == block
            motion = [jnp.where(here, moved[k, c], motion[c]) for c in range(6)]
            key = jnp.where(here, moved_keys[k], key)
        keep(block, motion, key)
        return carry

    def pair_block(tile, y, block, height, before):
        other = [jnp.broadcast_to(near[block, c, pl.ds(y, 1), :], (8, slots)) for c in range(7)]
        key = jnp.broadcast_to(near_keys[block, 0, pl.ds(y, 1), :], (8, slots))
        offset = jnp.broadcast_to(near_keys[block, 1, pl.ds(y, 1), :], (8, slots))
        even = other[6] < 0.5
        for g in range(0, height, 8):
            at = pl.ds(g, 8)
            own = [wide[tile, c, at, :] for c in range(8)]
            own_key, own_offset = wide_keys[tile, 0, at, :], wide_keys[tile, 1, at, :]
            terms = pair_strength(own, own_key, own_offset, own[6], own[7], other, key, offset, even)
            for c in range(3):
                forces[tile, c, at, :] = before[tile, c, at, :] + terms[c]

    def tile_pairs(tile, carry):
        y = tile % out_y
        blocks = limits[0, tile]
        heights = list(range(slots // 2, slots + 1, STEP))

        def at_height(height):
            def run():
                pair_block(tile, y, 0, height, own_forces)

                def one(block, carry):
                    pair_block(tile, y, block, height, forces)
                    return carry

                lax.fori_loop(1, blocks, one, 0)

            return run

        which = jnp.clip((limits[1, tile] + STEP - 1) // STEP - heights[0] // STEP, 0, len(heights) - 1)
        lax.switch(which, [at_height(h) for h in heights])
        return carry

    ones = jnp.ones((8, slots), jnp.bfloat16)
    for zz in range(out_z):
        z = gz * out_z + zz
        total = place_candidates(z)
        present = rows(0, 0, z, 0) < 0.5 * FAR
        blocks = jnp.maximum(1, (total.astype(jnp.int32) + (slots - 1)) >> lane_bits)
        count = jnp.sum(jnp.where(present, 1.0, 0.0), axis=1, keepdims=True).astype(jnp.int32)
        for y in range(out_y):
            limits[0, zz * out_y + y] = blocks[y, 0]
            limits[1, zz * out_y + y] = count[y, 0]
        lax.fori_loop(0, jnp.max(blocks), assemble, 0)
        lax.fori_loop(zz * out_y, (zz + 1) * out_y, tile_pairs, 0)
        for y in range(out_y):
            tile = zz * out_y + y
            for c in range(3):
                whole = forces[tile, c]
                high = whole.astype(jnp.bfloat16)
                low = (whole - high.astype(jnp.float32)).astype(jnp.bfloat16)
                kick = sum(
                    lax.dot_general(ones, part, (((1,), (1,)), ((), ())), preferred_element_type=jnp.float32)
                    for part in (high, low)
                )
                out_ref[c, 0, y, pl.ds(zz, 1), :] = jnp.where(present[y : y + 1], kick_scale * UNIT * kick[:1], 0.0)


def on_device(nx, ny, nz, positions, velocities, bead_keys, counts):
    _, _, block_y, tiles_z, slots = positions.shape
    out_y, out_z = block_y * nz, tiles_z // nz
    span = out_y + 2
    tiles = out_y * out_z
    gathered = pl.pallas_call(
        functools.partial(gather_kernel, (nx, ny, nz, block_y, tiles_z)),
        out_shape=[
            jax.ShapeDtypeStruct((3, span, tiles_z, ROWS, slots), jnp.float32),
            jax.ShapeDtypeStruct((tiles, 8, slots, slots), jnp.float32),
            jax.ShapeDtypeStruct((tiles, 2, slots, slots), jnp.int32),
            jax.ShapeDtypeStruct((tiles, 3, slots, slots), jnp.float32),
        ],
        in_specs=[pl.BlockSpec(memory_space=pltpu.HBM)] * 4,
        out_specs=[pl.BlockSpec(memory_space=pltpu.VMEM)] * 4,
        scratch_shapes=[
            pltpu.VMEM(positions.shape, jnp.float32),
            pltpu.VMEM(velocities.shape, jnp.float32),
            pltpu.VMEM(bead_keys.shape, jnp.int32),
            pltpu.SMEM((1, tiles_z, block_y), jnp.int32),
            pltpu.VMEM((block_y, tiles_z, ROWS, slots), jnp.float32),
            pltpu.VMEM((3 * ROWS, ROWS * slots), jnp.bfloat16),
            pltpu.SemaphoreType.DMA((3, nz)),
            pltpu.SemaphoreType.DMA((3, nz)),
            pltpu.SemaphoreType.DMA((2, 3, nz)),
            pltpu.SemaphoreType.DMA((2, 3)),
            pltpu.SemaphoreType.DMA,
            pltpu.SemaphoreType.DMA((4,)),
        ],
        compiler_params=pltpu.CompilerParams(
            collective_id=0, has_side_effects=True, vmem_limit_bytes=12582912
        ),
        name="gather_tiles",
    )(*(pltpu.with_memory_space_constraint(a, pltpu.HBM) for a in (positions, velocities, bead_keys, jnp.swapaxes(counts, 1, 2))))
    shells = len(shell_of(tiles_z))
    return pl.pallas_call(
        functools.partial(pair_kernel, (tiles_z, out_y, out_z)),
        out_shape=jax.ShapeDtypeStruct((3, 1, out_y, out_z, slots), jnp.float32),
        in_specs=[pl.BlockSpec(memory_space=pltpu.VMEM)] * 4,
        out_specs=pl.BlockSpec(memory_space=pltpu.VMEM),
        scratch_shapes=[
            pltpu.VMEM((shells * out_y, slots), jnp.float32),
            pltpu.VMEM((shells, out_y, slots), jnp.int32),
            pltpu.VMEM((shells, 6, out_y, slots), jnp.float32),
            pltpu.VMEM((shells, out_y, slots), jnp.int32),
            pltpu.VMEM((shells, 7, out_y, slots), jnp.float32),
            pltpu.VMEM((shells, 2, out_y, slots), jnp.int32),
            pltpu.VMEM((tiles, 3, slots, slots), jnp.float32),
            pltpu.SMEM((2, tiles), jnp.int32),
        ],
        compiler_params=pltpu.CompilerParams(vmem_limit_bytes=16777216),
        name="pair_kicks",
    )(*gathered)


def solution(mesh):
    in_specs = (
        P(None, "gx", ("gy", "gz"), None, None),
        P(None, "gx", ("gy", "gz"), None, None),
        P("gx", ("gy", "gz"), None, None),
        P("gx", ("gy", "gz"), None),
    )
    out_specs = P(None, "gx", "gy", "gz", None)
    nx, ny, nz = mesh.shape["gx"], mesh.shape["gy"], mesh.shape["gz"]
    return jax.shard_map(
        functools.partial(on_device, nx, ny, nz),
        mesh=mesh,
        in_specs=in_specs,
        out_specs=out_specs,
        check_vma=False,
    )
```

```python
import functools

import jax
import jax.numpy as jnp
from jax import lax
from jax.experimental import pallas as pl
from jax.experimental.pallas import tpu as pltpu
from jax.sharding import PartitionSpec as P

SIDE = 3.0

soft_radius = 0.05
friction = 4.5
noise_amplitude = 15.0
like_repulsion = 25.0
unlike_extra = 15.0
kick_scale = 0.02
root_twelve = 3.4641016151377544

FAR = 1.0e9
ROWS = 8
KEY_A = 1103515245
KEY_B = 12345
KEY_C = 747796405
STEP = 16
REACH = 1.00001
UNIT = noise_amplitude * root_twelve / 2147483648.0
MESH = pl.DeviceIdType.MESH


def pair_strength(own, own_key, own_offset, own_even, own_odd, other, key, offset, even):
    sep = [own[c] - other[c] for c in range(3)]
    squared = sep[0] * sep[0] + sep[1] * sep[1] + sep[2] * sep[2]
    root = lax.rsqrt(jnp.maximum(squared, 1e-30))
    scaled = jnp.maximum(1.0 - squared * root, 0.0) * jnp.minimum(root, 1.0 / soft_radius)
    dot = sep[0] * (own[3] - other[3]) + sep[1] * (own[4] - other[4]) + sep[2] * (own[5] - other[5])
    hashed = (own_key ^ key) * KEY_A + (own_offset + offset)
    hashed = hashed ^ lax.shift_right_logical(hashed, 15)
    hashed = hashed * KEY_C
    hashed = hashed ^ lax.shift_right_logical(hashed, 13)
    push = (hashed & 0x7FFFFF80).astype(jnp.float32) + jnp.where(even, own_even, own_odd)
    strength = scaled * (push - scaled * dot)
    return [strength * part for part in sep]


def split(values):
    high = values.astype(jnp.bfloat16).astype(jnp.float32)
    middle = (values - high).astype(jnp.bfloat16).astype(jnp.float32)
    return [high, middle, values - high - middle]


def column_of(tiles_z):
    return [None] if tiles_z == 2 else [-1, 1]


def own_tile(tile, column, z, select, wide, wide_keys, forces):
    tiles_z, _, slots = column.shape
    rows = column[z]
    parts = split(rows)
    spread = jnp.dot(jnp.transpose(jnp.concatenate(parts, axis=0)).astype(jnp.bfloat16), select[...], preferred_element_type=jnp.float32)

    def side(dz):
        near = rows if dz == 0 else column[1 - z if dz is None else lax.rem(z + dz + tiles_z, tiles_z)]
        motion = [near[c : c + 1] for c in range(6)]
        if dz is None:
            motion[2] = motion[2] + jnp.where(motion[2] < 0.5 * SIDE, SIDE, -SIDE)
        else:
            motion[2] = motion[2] + SIDE * dz
        key = near[6:7].astype(jnp.int32) * 32768 + near[7:8].astype(jnp.int32)
        motion, key = [jnp.broadcast_to(m, (8, slots)) for m in motion], jnp.broadcast_to(key, (8, slots))
        return motion, key, key * KEY_B, (key & 1) == 0

    sides = [side(dz) for dz in [0] + column_of(tiles_z)]
    level = (like_repulsion - 0.5 * noise_amplitude * root_twelve) / UNIT
    for g in range(0, slots, 8):
        at = pl.ds(g, 8)
        part = [spread[g : g + 8, c * slots : (c + 1) * slots] for c in range(8)]
        low = part[7].astype(jnp.int32)
        own_key = part[6].astype(jnp.int32) * 32768 + low
        own_offset = own_key * KEY_B
        kind = (low & 1).astype(jnp.float32) * (unlike_extra / UNIT)
        own_even = level + kind
        own_odd = (level + unlike_extra / UNIT) - kind
        for c in range(6):
            wide[tile, c, at, :] = part[c]
        wide[tile, 6, at, :] = own_even
        wide[tile, 7, at, :] = own_odd
        wide_keys[tile, 0, at, :] = own_key
        wide_keys[tile, 1, at, :] = own_offset
        terms = [pair_strength(part, own_key, own_offset, own_even, own_odd, *one) for one in sides]
        for c in range(3):
            forces[tile, c, at, :] = functools.reduce(jnp.add, [term[c] for term in terms])


def gather_kernel(sizes, pos_in, vel_in, key_in, count_in, all_ref, wide, wide_keys, forces, below, pos_ref, vel_ref, key_ref, count_ref, packed, select, send, recv, edge_send, edge_recv, local, loads):
    nx, ny, nz, block_y, tiles_z = sizes
    gx, gy, gz = lax.axis_index("gx"), lax.axis_index("gy"), lax.axis_index("gz")
    slots = pos_ref.shape[-1]
    inputs = ((pos_in, pos_ref), (vel_in, vel_ref), (key_in, key_ref), (count_in, count_ref))
    fetches = [pltpu.make_async_copy(a, b, loads.at[k]) for k, (a, b) in enumerate(inputs)]
    for fetch in fetches:
        fetch.start()
    top = nz * block_y + 1
    barrier = pltpu.get_barrier_semaphore()

    def target(e, group, member):
        return (lax.rem(gx + e + nx, nx), lax.rem(gy + group + ny, ny), lax.rem(member + nz, nz))

    steps = (-1, 0, 1)
    for e in steps:
        for r in range(nz):
            if e or r:
                pl.semaphore_signal(barrier, inc=1, device_id=target(e, 0, gz + r), device_id_type=MESH)
        pl.semaphore_signal(barrier, inc=1, device_id=target(e, -1, nz - 1), device_id_type=MESH)
        pl.semaphore_signal(barrier, inc=1, device_id=target(e, 1, 0), device_id_type=MESH)

    row = lax.broadcasted_iota(jnp.int32, select.shape, 0)
    column = lax.broadcasted_iota(jnp.int32, select.shape, 1)
    chosen = (row & (ROWS - 1)) == (column >> (slots - 1).bit_length())
    select[...] = jnp.where(chosen, 1.0, 0.0).astype(jnp.bfloat16)
    lane_bits = (slots - 1).bit_length()
    row = lax.broadcasted_iota(jnp.int32, below.shape, 0)
    column = lax.broadcasted_iota(jnp.int32, below.shape, 1)
    limit = jnp.where(column < slots, column + 1, (column >> lane_bits) * (slots // 4))
    below[...] = jnp.where(row < limit, 1.0, 0.0).astype(jnp.bfloat16)
    for fetch in fetches:
        fetch.wait()
    lane = lax.broadcasted_iota(jnp.int32, (1, slots), 1)
    for y in range(block_y):
        for z in range(tiles_z):
            present = lane < count_ref[0, z, y]
            key = key_ref[0, y, pl.ds(z, 1), :]
            rows = [jnp.where(present, pos_ref[c, 0, y, pl.ds(z, 1), :], FAR) for c in range(3)]
            rows += [vel_ref[c, 0, y, pl.ds(z, 1), :] * (friction / UNIT) for c in range(3)]
            rows += [(key >> 15).astype(jnp.float32), (key & 32767).astype(jnp.float32)]
            packed[y, z] = jnp.concatenate(rows, axis=0)

    def group_copy(e, r, slot_of):
        return pltpu.make_async_remote_copy(
            src_ref=packed,
            dst_ref=all_ref.at[1 - e, pl.ds(1 + slot_of * block_y, block_y)],
            send_sem=send.at[e + 1, r],
            recv_sem=recv.at[e + 1, r],
            device_id=target(e, 0, gz + r),
            device_id_type=MESH,
        )

    def edge_copy(e, side, member):
        first = side == 0
        return pltpu.make_async_remote_copy(
            src_ref=packed.at[pl.ds(0 if first else block_y - 1, 1)],
            dst_ref=all_ref.at[1 - e, pl.ds(top if first else 0, 1)],
            send_sem=edge_send.at[side, e + 1, member],
            recv_sem=edge_recv.at[side, e + 1],
            device_id=target(e, -1 if first else 1, member),
            device_id_type=MESH,
        )

    ends = jnp.where(gz == 0, 1, 0) + jnp.where(gz == nz - 1, 1, 0)
    pl.semaphore_wait(barrier, 3 * nz - 1 + 3 * nz * ends)

    def edges(side, act):
        for e in (-1, 1, 0):
            for member in range(nz):
                act(edge_copy(e, side, member))

    @pl.when(gz == 0)
    def _():
        edges(0, lambda c: c.start())

    @pl.when(gz == nz - 1)
    def _():
        edges(1, lambda c: c.start())

    for r in reversed(range(nz)):
        for e in (0, -1, 1):
            if e or r:
                group_copy(e, r, gz).start()

    mine = pltpu.make_async_copy(packed, all_ref.at[1, pl.ds(1 + gz * block_y, block_y)], local)
    mine.start()
    out_y, out_z = nz * block_y, tiles_z // nz
    for zz in range(out_z):

        def near_one(y, carry, zz=zz):
            own_tile(zz * out_y + gz * block_y + y, packed.at[y], gz * out_z + zz, select, wide, wide_keys, forces)
            return carry

        lax.fori_loop(0, block_y, near_one, 0, unroll=min(2, block_y))

    for r in range(1, nz):
        slot_of = lax.rem(gz - r + nz, nz)
        group_copy(0, r, slot_of).wait_recv()
        for zz in range(out_z):

            def remote(y, carry, zz=zz, slot_of=slot_of):
                at = slot_of * block_y + y
                own_tile(zz * out_y + at, all_ref.at[1, 1 + at], gz * out_z + zz, select, wide, wide_keys, forces)
                return carry

            lax.fori_loop(0, block_y, remote, 0, unroll=min(2, block_y))

    mine.wait()
    for e in steps:
        for r in range(nz):
            if e or r:
                copy = group_copy(e, r, lax.rem(gz - r + nz, nz))
                if e:
                    copy.wait_recv()
                copy.wait_send()
        for side in range(2):
            edge_copy(e, side, 0).wait_recv()

    @pl.when(gz == 0)
    def _():
        edges(0, lambda c: c.wait_send())

    @pl.when(gz == nz - 1)
    def _():
        edges(1, lambda c: c.wait_send())


def shell_of(tiles_z):
    layers = (0, None) if tiles_z == 2 else (-1, 0, 1)
    offsets = [(dx, dy, dz) for dx in (-1, 0, 1) for dy in (-1, 0, 1) for dz in layers]
    done = [(0, 0, dz) for dz in [0] + column_of(tiles_z)]
    return [offset for offset in offsets if offset not in done]


def pair_kernel(sizes, all_ref, wide, wide_keys, own_forces, below, out_ref, masks, places, moved, moved_keys, near, near_keys, forces, limits):
    tiles_z, out_y, out_z = sizes
    slots = all_ref.shape[-1]
    span = all_ref.shape[1]
    gz = lax.axis_index("gz")
    shell = shell_of(tiles_z)
    n = len(shell)
    lane_bits = (slots - 1).bit_length()
    quarter = slots // 4
    flat = all_ref.reshape(3 * span * tiles_z * ROWS, slots)
    lane = lax.broadcasted_iota(jnp.int32, (out_y, slots), 1)

    def rows(dx, dy, z, c):
        start = (((1 + dx) * span + 1 + dy) * tiles_z + z) * ROWS + c
        return flat[pl.ds(start, out_y, stride=tiles_z * ROWS), :]

    def keys_of(dx, dy, z):
        return rows(dx, dy, z, 6).astype(jnp.int32) * 32768 + rows(dx, dy, z, 7).astype(jnp.int32)

    def place_candidates(z):
        def position(k):
            dx, dy, dz = shell[k]
            other = 1 - z if dz is None else lax.rem(z + dz + tiles_z, tiles_z)
            p = [rows(dx, dy, other, c) for c in range(3)]
            if dx:
                p[0] = p[0] + SIDE * dx
            if dy:
                p[1] = p[1] + SIDE * dy
            if dz is None:
                p[2] = p[2] + jnp.where(p[2] < 0.5 * SIDE, SIDE, -SIDE)
            elif dz:
                p[2] = p[2] + SIDE * dz
            return p, other

        for k in range(n):
            dx, dy, dz = shell[k]
            other = 1 - z if dz is None else lax.rem(z + dz + tiles_z, tiles_z)
            gap = None
            for c, side in enumerate((dx, dy, dz)):
                if side != 0:
                    value = rows(dx, dy, other, c)
                    if side is None:
                        value = jnp.minimum(value, SIDE - value)
                    elif side < 0:
                        value = SIDE - value
                    gap = value * value if gap is None else gap + value * value
            masks[pl.ds(k * out_y, out_y), :] = jnp.where(gap < REACH, 1.0, 0.0)

        sums = jnp.dot(masks[...].astype(jnp.bfloat16), below[...], preferred_element_type=jnp.float32)
        start = jnp.zeros((out_y, slots), jnp.float32)
        for k in range(n):
            part = [sums[k * out_y : (k + 1) * out_y, q * slots : (q + 1) * slots] for q in range(5)]
            first = start.astype(jnp.int32)
            want = (lane - first) & (slots - 1)
            level = want.astype(jnp.float32)
            at = jnp.where(
                part[2] <= level,
                jnp.where(part[3] <= level, 3 * quarter, 2 * quarter),
                jnp.where(part[1] <= level, quarter, 0),
            )
            bit = quarter // 2
            while bit:
                seen = jnp.take_along_axis(part[0], at + (bit - 1), axis=1, mode="promise_in_bounds")
                at = jnp.where(seen <= level, at + bit, at)
                bit //= 2
            places[k] = jnp.where(level < part[4], (first + want) >> lane_bits, -1)
            start = start + part[4]
            p, other = position(k)
            dx, dy, _ = shell[k]
            p += [rows(dx, dy, other, c) for c in range(3, 6)]
            for c in range(6):
                moved[k, c] = jnp.take_along_axis(p[c], at, axis=1, mode="promise_in_bounds")
            moved_keys[k] = jnp.take_along_axis(keys_of(dx, dy, other), at, axis=1, mode="promise_in_bounds")
        return start

    def keep(block, motion, key):
        for c in range(6):
            near[block, c] = motion[c]
        near[block, 6] = (key & 1).astype(jnp.float32)
        near_keys[block, 0] = key
        near_keys[block, 1] = key * KEY_B

    def assemble(block, carry):
        motion = [jnp.full((out_y, slots), FAR if c < 3 else 0.0, jnp.float32) for c in range(6)]
        key = jnp.zeros((out_y, slots), jnp.int32)
        for k in range(n):
            here = places[k] == block
            motion = [jnp.where(here, moved[k, c], motion[c]) for c in range(6)]
            key = jnp.where(here, moved_keys[k], key)
        keep(block, motion, key)
        return carry

    def pair_block(tile, y, block, height, before):
        other = [jnp.broadcast_to(near[block, c, pl.ds(y, 1), :], (8, slots)) for c in range(7)]
        key = jnp.broadcast_to(near_keys[block, 0, pl.ds(y, 1), :], (8, slots))
        offset = jnp.broadcast_to(near_keys[block, 1, pl.ds(y, 1), :], (8, slots))
        even = other[6] < 0.5
        for g in range(0, height, 8):
            at = pl.ds(g, 8)
            own = [wide[tile, c, at, :] for c in range(8)]
            own_key, own_offset = wide_keys[tile, 0, at, :], wide_keys[tile, 1, at, :]
            terms = pair_strength(own, own_key, own_offset, own[6], own[7], other, key, offset, even)
            for c in range(3):
                forces[tile, c, at, :] = before[tile, c, at, :] + terms[c]

    def tile_pairs(tile, carry):
        y = tile % out_y
        blocks = limits[0, tile]
        heights = list(range(slots // 2, slots + 1, STEP))

        def at_height(height):
            def run():
                pair_block(tile, y, 0, height, own_forces)

                def one(block, carry):
                    pair_block(tile, y, block, height, forces)
                    return carry

                lax.fori_loop(1, blocks, one, 0)

            return run

        which = jnp.clip((limits[1, tile] + STEP - 1) // STEP - heights[0] // STEP, 0, len(heights) - 1)
        lax.switch(which, [at_height(h) for h in heights])
        return carry

    ones = jnp.ones((2 * slots, slots), jnp.bfloat16)
    wide_lane = lax.broadcasted_iota(jnp.int32, (slots, slots), 1)
    for zz in range(out_z):
        z = gz * out_z + zz
        total = place_candidates(z)
        present = rows(0, 0, z, 0) < 0.5 * FAR
        blocks = jnp.maximum(1, (total.astype(jnp.int32) + (slots - 1)) >> lane_bits)
        count = jnp.sum(jnp.where(present, 1.0, 0.0), axis=1, keepdims=True).astype(jnp.int32)
        for y in range(out_y):
            limits[0, zz * out_y + y] = blocks[y, 0]
            limits[1, zz * out_y + y] = count[y, 0]
        lax.fori_loop(0, jnp.max(blocks), assemble, 0)
        lax.fori_loop(zz * out_y, (zz + 1) * out_y, tile_pairs, 0)
        total = jnp.zeros((slots, slots), jnp.float32)
        for y in range(out_y):
            for c in range(3):
                whole = forces[zz * out_y + y, c]
                high = whole.astype(jnp.bfloat16)
                low = (whole - high.astype(jnp.float32)).astype(jnp.bfloat16)
                sums = jnp.dot(jnp.concatenate([high, low], axis=1), ones, preferred_element_type=jnp.float32)
                total = jnp.where(wide_lane == c * out_y + y, sums, total)
        kicks = jnp.transpose(total)
        for c in range(3):
            kick = jnp.where(present, kick_scale * UNIT * kicks[c * out_y : (c + 1) * out_y], 0.0)
            for y in range(out_y):
                out_ref[c, 0, y, pl.ds(zz, 1), :] = kick[y : y + 1]


def on_device(nx, ny, nz, positions, velocities, bead_keys, counts):
    _, _, block_y, tiles_z, slots = positions.shape
    out_y, out_z = block_y * nz, tiles_z // nz
    span = out_y + 2
    tiles = out_y * out_z
    gathered = pl.pallas_call(
        functools.partial(gather_kernel, (nx, ny, nz, block_y, tiles_z)),
        out_shape=[
            jax.ShapeDtypeStruct((3, span, tiles_z, ROWS, slots), jnp.float32),
            jax.ShapeDtypeStruct((tiles, 8, slots, slots), jnp.float32),
            jax.ShapeDtypeStruct((tiles, 2, slots, slots), jnp.int32),
            jax.ShapeDtypeStruct((tiles, 3, slots, slots), jnp.float32),
            jax.ShapeDtypeStruct((slots, 5 * slots), jnp.bfloat16),
        ],
        in_specs=[pl.BlockSpec(memory_space=pltpu.HBM)] * 4,
        out_specs=[pl.BlockSpec(memory_space=pltpu.VMEM)] * 5,
        scratch_shapes=[
            pltpu.VMEM(positions.shape, jnp.float32),
            pltpu.VMEM(velocities.shape, jnp.float32),
            pltpu.VMEM(bead_keys.shape, jnp.int32),
            pltpu.SMEM((1, tiles_z, block_y), jnp.int32),
            pltpu.VMEM((block_y, tiles_z, ROWS, slots), jnp.float32),
            pltpu.VMEM((3 * ROWS, ROWS * slots), jnp.bfloat16),
            pltpu.SemaphoreType.DMA((3, nz)),
            pltpu.SemaphoreType.DMA((3, nz)),
            pltpu.SemaphoreType.DMA((2, 3, nz)),
            pltpu.SemaphoreType.DMA((2, 3)),
            pltpu.SemaphoreType.DMA,
            pltpu.SemaphoreType.DMA((4,)),
        ],
        compiler_params=pltpu.CompilerParams(
            collective_id=0, has_side_effects=True, vmem_limit_bytes=12582912
        ),
        name="gather_tiles",
    )(*(pltpu.with_memory_space_constraint(a, pltpu.HBM) for a in (positions, velocities, bead_keys, jnp.swapaxes(counts, 1, 2))))
    shells = len(shell_of(tiles_z))
    return pl.pallas_call(
        functools.partial(pair_kernel, (tiles_z, out_y, out_z)),
        out_shape=jax.ShapeDtypeStruct((3, 1, out_y, out_z, slots), jnp.float32),
        in_specs=[pl.BlockSpec(memory_space=pltpu.VMEM)] * 5,
        out_specs=pl.BlockSpec(memory_space=pltpu.VMEM),
        scratch_shapes=[
            pltpu.VMEM((shells * out_y, slots), jnp.float32),
            pltpu.VMEM((shells, out_y, slots), jnp.int32),
            pltpu.VMEM((shells, 6, out_y, slots), jnp.float32),
            pltpu.VMEM((shells, out_y, slots), jnp.int32),
            pltpu.VMEM((shells, 7, out_y, slots), jnp.float32),
            pltpu.VMEM((shells, 2, out_y, slots), jnp.int32),
            pltpu.VMEM((tiles, 3, slots, slots), jnp.float32),
            pltpu.SMEM((2, tiles), jnp.int32),
        ],
        compiler_params=pltpu.CompilerParams(vmem_limit_bytes=16777216),
        name="pair_kicks",
    )(*gathered)


def solution(mesh):
    in_specs = (
        P(None, "gx", ("gy", "gz"), None, None),
        P(None, "gx", ("gy", "gz"), None, None),
        P("gx", ("gy", "gz"), None, None),
        P("gx", ("gy", "gz"), None),
    )
    out_specs = P(None, "gx", "gy", "gz", None)
    nx, ny, nz = mesh.shape["gx"], mesh.shape["gy"], mesh.shape["gz"]
    return jax.shard_map(
        functools.partial(on_device, nx, ny, nz),
        mesh=mesh,
        in_specs=in_specs,
        out_specs=out_specs,
        check_vma=False,
    )
```

```python
import functools

import jax
import jax.numpy as jnp
from jax import lax
from jax.experimental import pallas as pl
from jax.experimental.pallas import tpu as pltpu
from jax.sharding import PartitionSpec as P

SIDE = 3.0

soft_radius = 0.05
friction = 4.5
noise_amplitude = 15.0
like_repulsion = 25.0
unlike_extra = 15.0
kick_scale = 0.02
root_twelve = 3.4641016151377544

FAR = 1.0e9
ROWS = 8
KEY_A = 1103515245
KEY_B = 12345
KEY_C = 747796405
STEP = 16
REACH = 1.00001
UNIT = noise_amplitude * root_twelve / 2147483648.0
MESH = pl.DeviceIdType.MESH


def pair_strength(own, own_key, own_offset, own_even, own_odd, other, key, offset, even):
    sep = [own[c] - other[c] for c in range(3)]
    squared = sep[0] * sep[0] + sep[1] * sep[1] + sep[2] * sep[2]
    root = lax.rsqrt(jnp.maximum(squared, 1e-30))
    scaled = jnp.maximum(1.0 - squared * root, 0.0) * jnp.minimum(root, 1.0 / soft_radius)
    dot = sep[0] * (own[3] - other[3]) + sep[1] * (own[4] - other[4]) + sep[2] * (own[5] - other[5])
    hashed = (own_key ^ key) * KEY_A + (own_offset + offset)
    hashed = hashed ^ lax.shift_right_logical(hashed, 15)
    hashed = hashed * KEY_C
    hashed = hashed ^ lax.shift_right_logical(hashed, 13)
    push = (hashed & 0x7FFFFF80).astype(jnp.float32) + jnp.where(even, own_even, own_odd)
    strength = scaled * (push - scaled * dot)
    return [strength * part for part in sep]


def split(values):
    high = values.astype(jnp.bfloat16).astype(jnp.float32)
    middle = (values - high).astype(jnp.bfloat16).astype(jnp.float32)
    return [high, middle, values - high - middle]


def column_of(tiles_z):
    return [None] if tiles_z == 2 else [-1, 1]


def own_tile(tile, brick, y, z, paired, select, wide, wide_keys, forces):
    block_y, tiles_z, _, slots = brick.shape
    column = brick.at[y]
    rows = column[z]
    parts = split(rows)
    spread = jnp.dot(jnp.transpose(jnp.concatenate(parts, axis=0)).astype(jnp.bfloat16), select[...], preferred_element_type=jnp.float32)

    def side(near, dz, shift_y=None):
        motion = [near[c : c + 1] for c in range(6)]
        if dz is None:
            motion[2] = motion[2] + jnp.where(motion[2] < 0.5 * SIDE, SIDE, -SIDE)
        elif dz:
            motion[2] = motion[2] + SIDE * dz
        if shift_y is not None:
            motion[1] = motion[1] + shift_y
        key = near[6:7].astype(jnp.int32) * 32768 + near[7:8].astype(jnp.int32)
        motion, key = [jnp.broadcast_to(m, (8, slots)) for m in motion], jnp.broadcast_to(key, (8, slots))
        return motion, key, key * KEY_B, (key & 1) == 0

    sides = [side(rows, 0)]
    for dz in column_of(tiles_z):
        sides.append(side(column[1 - z if dz is None else lax.rem(z + dz + tiles_z, tiles_z)], dz))
    if paired and block_y > 1:
        step = 1 - 2 * (y // (block_y // 2))
        sides.append(side(brick[y + step, z], 0, step.astype(jnp.float32) * SIDE))
    level = (like_repulsion - 0.5 * noise_amplitude * root_twelve) / UNIT
    for g in range(0, slots, 8):
        at = pl.ds(g, 8)
        part = [spread[g : g + 8, c * slots : (c + 1) * slots] for c in range(8)]
        low = part[7].astype(jnp.int32)
        own_key = part[6].astype(jnp.int32) * 32768 + low
        own_offset = own_key * KEY_B
        kind = (low & 1).astype(jnp.float32) * (unlike_extra / UNIT)
        own_even = level + kind
        own_odd = (level + unlike_extra / UNIT) - kind
        for c in range(6):
            wide[tile, c, at, :] = part[c]
        wide[tile, 6, at, :] = own_even
        wide[tile, 7, at, :] = own_odd
        wide_keys[tile, 0, at, :] = own_key
        wide_keys[tile, 1, at, :] = own_offset
        terms = [pair_strength(part, own_key, own_offset, own_even, own_odd, *one) for one in sides]
        for c in range(3):
            forces[tile, c, at, :] = functools.reduce(jnp.add, [term[c] for term in terms])


def gather_kernel(sizes, pos_in, vel_in, key_in, count_in, all_ref, wide, wide_keys, forces, below, pos_ref, vel_ref, key_ref, count_ref, packed, select, send, recv, edge_send, edge_recv, local, loads):
    nx, ny, nz, block_y, tiles_z = sizes
    gx, gy, gz = lax.axis_index("gx"), lax.axis_index("gy"), lax.axis_index("gz")
    slots = pos_ref.shape[-1]
    inputs = ((pos_in, pos_ref), (vel_in, vel_ref), (key_in, key_ref), (count_in, count_ref))
    fetches = [pltpu.make_async_copy(a, b, loads.at[k]) for k, (a, b) in enumerate(inputs)]
    for fetch in fetches:
        fetch.start()
    top = nz * block_y + 1
    barrier = pltpu.get_barrier_semaphore()

    def target(e, group, member):
        return (lax.rem(gx + e + nx, nx), lax.rem(gy + group + ny, ny), lax.rem(member + nz, nz))

    steps = (-1, 0, 1)
    for e in steps:
        for r in range(nz):
            if e or r:
                pl.semaphore_signal(barrier, inc=1, device_id=target(e, 0, gz + r), device_id_type=MESH)
        pl.semaphore_signal(barrier, inc=1, device_id=target(e, -1, nz - 1), device_id_type=MESH)
        pl.semaphore_signal(barrier, inc=1, device_id=target(e, 1, 0), device_id_type=MESH)

    row = lax.broadcasted_iota(jnp.int32, select.shape, 0)
    column = lax.broadcasted_iota(jnp.int32, select.shape, 1)
    chosen = (row & (ROWS - 1)) == (column >> (slots - 1).bit_length())
    select[...] = jnp.where(chosen, 1.0, 0.0).astype(jnp.bfloat16)
    lane_bits = (slots - 1).bit_length()
    row = lax.broadcasted_iota(jnp.int32, below.shape, 0)
    column = lax.broadcasted_iota(jnp.int32, below.shape, 1)
    limit = jnp.where(column < slots, column + 1, (column >> lane_bits) * (slots // 4))
    below[...] = jnp.where(row < limit, 1.0, 0.0).astype(jnp.bfloat16)
    for fetch in fetches:
        fetch.wait()
    lane = lax.broadcasted_iota(jnp.int32, (1, slots), 1)
    for y in range(block_y):
        for z in range(tiles_z):
            present = lane < count_ref[0, z, y]
            key = key_ref[0, y, pl.ds(z, 1), :]
            rows = [jnp.where(present, pos_ref[c, 0, y, pl.ds(z, 1), :], FAR) for c in range(3)]
            rows += [vel_ref[c, 0, y, pl.ds(z, 1), :] * (friction / UNIT) for c in range(3)]
            rows += [(key >> 15).astype(jnp.float32), (key & 32767).astype(jnp.float32)]
            packed[y, z] = jnp.concatenate(rows, axis=0)

    def group_copy(e, r, slot_of):
        return pltpu.make_async_remote_copy(
            src_ref=packed,
            dst_ref=all_ref.at[1 - e, pl.ds(1 + slot_of * block_y, block_y)],
            send_sem=send.at[e + 1, r],
            recv_sem=recv.at[e + 1, r],
            device_id=target(e, 0, gz + r),
            device_id_type=MESH,
        )

    def edge_copy(e, side, member):
        first = side == 0
        return pltpu.make_async_remote_copy(
            src_ref=packed.at[pl.ds(0 if first else block_y - 1, 1)],
            dst_ref=all_ref.at[1 - e, pl.ds(top if first else 0, 1)],
            send_sem=edge_send.at[side, e + 1, member],
            recv_sem=edge_recv.at[side, e + 1],
            device_id=target(e, -1 if first else 1, member),
            device_id_type=MESH,
        )

    ends = jnp.where(gz == 0, 1, 0) + jnp.where(gz == nz - 1, 1, 0)
    pl.semaphore_wait(barrier, 3 * nz - 1 + 3 * nz * ends)

    def edges(side, act):
        for e in (-1, 1, 0):
            for member in range(nz):
                act(edge_copy(e, side, member))

    @pl.when(gz == 0)
    def _():
        edges(0, lambda c: c.start())

    @pl.when(gz == nz - 1)
    def _():
        edges(1, lambda c: c.start())

    for r in reversed(range(nz)):
        for e in (0, -1, 1):
            if e or r:
                group_copy(e, r, gz).start()

    mine = pltpu.make_async_copy(packed, all_ref.at[1, pl.ds(1 + gz * block_y, block_y)], local)
    mine.start()
    out_y, out_z = nz * block_y, tiles_z // nz
    for zz in range(out_z):

        def near_one(y, carry, zz=zz):
            own_tile(zz * out_y + gz * block_y + y, packed, y, gz * out_z + zz, True, select, wide, wide_keys, forces)
            return carry

        lax.fori_loop(0, block_y, near_one, 0, unroll=min(2, block_y))

    for r in range(1, nz):
        slot_of = lax.rem(gz - r + nz, nz)
        group_copy(0, r, slot_of).wait_recv()
        for zz in range(out_z):

            def remote(y, carry, zz=zz, slot_of=slot_of):
                at = slot_of * block_y + y
                own_tile(zz * out_y + at, all_ref.at[1, pl.ds(1 + slot_of * block_y, block_y)], y, gz * out_z + zz, False, select, wide, wide_keys, forces)
                return carry

            lax.fori_loop(0, block_y, remote, 0, unroll=min(2, block_y))

    mine.wait()
    for e in steps:
        for r in range(nz):
            if e or r:
                copy = group_copy(e, r, lax.rem(gz - r + nz, nz))
                if e:
                    copy.wait_recv()
                copy.wait_send()
        for side in range(2):
            edge_copy(e, side, 0).wait_recv()

    @pl.when(gz == 0)
    def _():
        edges(0, lambda c: c.wait_send())

    @pl.when(gz == nz - 1)
    def _():
        edges(1, lambda c: c.wait_send())


def shell_of(tiles_z):
    layers = (0, None) if tiles_z == 2 else (-1, 0, 1)
    offsets = [(dx, dy, dz) for dx in (-1, 0, 1) for dy in (-1, 0, 1) for dz in layers]
    done = [(0, 0, dz) for dz in [0] + column_of(tiles_z)]
    return [offset for offset in offsets if offset not in done]


def pair_kernel(sizes, all_ref, wide, wide_keys, own_forces, below, out_ref, masks, places, moved, moved_keys, near, near_keys, forces, limits):
    tiles_z, block_y, out_y, out_z = sizes
    slots = all_ref.shape[-1]
    span = all_ref.shape[1]
    gz = lax.axis_index("gz")
    shell = shell_of(tiles_z)
    n = len(shell)
    lane_bits = (slots - 1).bit_length()
    quarter = slots // 4
    flat = all_ref.reshape(3 * span * tiles_z * ROWS, slots)
    lane = lax.broadcasted_iota(jnp.int32, (out_y, slots), 1)
    line = lax.broadcasted_iota(jnp.int32, (out_y, slots), 0)

    def rows(dx, dy, z, c):
        start = (((1 + dx) * span + 1 + dy) * tiles_z + z) * ROWS + c
        return flat[pl.ds(start, out_y, stride=tiles_z * ROWS), :]

    def keys_of(dx, dy, z):
        return rows(dx, dy, z, 6).astype(jnp.int32) * 32768 + rows(dx, dy, z, 7).astype(jnp.int32)

    def place_candidates(z):
        def position(k):
            dx, dy, dz = shell[k]
            other = 1 - z if dz is None else lax.rem(z + dz + tiles_z, tiles_z)
            p = [rows(dx, dy, other, c) for c in range(3)]
            if dx:
                p[0] = p[0] + SIDE * dx
            if dy:
                p[1] = p[1] + SIDE * dy
            if dz is None:
                p[2] = p[2] + jnp.where(p[2] < 0.5 * SIDE, SIDE, -SIDE)
            elif dz:
                p[2] = p[2] + SIDE * dz
            return p, other

        for k in range(n):
            dx, dy, dz = shell[k]
            other = 1 - z if dz is None else lax.rem(z + dz + tiles_z, tiles_z)
            gap = None
            for c, side in enumerate((dx, dy, dz)):
                if side != 0:
                    value = rows(dx, dy, other, c)
                    if side is None:
                        value = jnp.minimum(value, SIDE - value)
                    elif side < 0:
                        value = SIDE - value
                    gap = value * value if gap is None else gap + value * value
            inside = gap < REACH
            if dx == 0 and dz == 0 and block_y > 1:
                step = 1 - 2 * ((line % block_y) // (block_y // 2))
                inside = inside & ((step != dy) | (line < gz * block_y) | (line >= (gz + 1) * block_y))
            masks[pl.ds(k * out_y, out_y), :] = jnp.where(inside, 1.0, 0.0)

        sums = jnp.dot(masks[...].astype(jnp.bfloat16), below[...], preferred_element_type=jnp.float32)
        start = jnp.zeros((out_y, slots), jnp.float32)
        for k in range(n):
            part = [sums[k * out_y : (k + 1) * out_y, q * slots : (q + 1) * slots] for q in range(5)]
            first = start.astype(jnp.int32)
            want = (lane - first) & (slots - 1)
            level = want.astype(jnp.float32)
            at = jnp.where(
                part[2] <= level,
                jnp.where(part[3] <= level, 3 * quarter, 2 * quarter),
                jnp.where(part[1] <= level, quarter, 0),
            )
            bit = quarter // 2
            while bit:
                seen = jnp.take_along_axis(part[0], at + (bit - 1), axis=1, mode="promise_in_bounds")
                at = jnp.where(seen <= level, at + bit, at)
                bit //= 2
            places[k] = jnp.where(level < part[4], (first + want) >> lane_bits, -1)
            start = start + part[4]
            p, other = position(k)
            dx, dy, _ = shell[k]
            p += [rows(dx, dy, other, c) for c in range(3, 6)]
            for c in range(6):
                moved[k, c] = jnp.take_along_axis(p[c], at, axis=1, mode="promise_in_bounds")
            moved_keys[k] = jnp.take_along_axis(keys_of(dx, dy, other), at, axis=1, mode="promise_in_bounds")
        return start

    def keep(block, motion, key):
        for c in range(6):
            near[block, c] = motion[c]
        near[block, 6] = (key & 1).astype(jnp.float32)
        near_keys[block, 0] = key
        near_keys[block, 1] = key * KEY_B

    def assemble(block, carry):
        motion = [jnp.full((out_y, slots), FAR if c < 3 else 0.0, jnp.float32) for c in range(6)]
        key = jnp.zeros((out_y, slots), jnp.int32)
        for k in range(n):
            here = places[k] == block
            motion = [jnp.where(here, moved[k, c], motion[c]) for c in range(6)]
            key = jnp.where(here, moved_keys[k], key)
        keep(block, motion, key)
        return carry

    def pair_blocks(tile, y, blocks, height, before):
        sides = []
        for block in blocks:
            other = [jnp.broadcast_to(near[block, c, pl.ds(y, 1), :], (8, slots)) for c in range(7)]
            key = jnp.broadcast_to(near_keys[block, 0, pl.ds(y, 1), :], (8, slots))
            offset = jnp.broadcast_to(near_keys[block, 1, pl.ds(y, 1), :], (8, slots))
            sides.append((other, key, offset, other[6] < 0.5))
        for g in range(0, height, 8):
            at = pl.ds(g, 8)
            own = [wide[tile, c, at, :] for c in range(8)]
            own_key, own_offset = wide_keys[tile, 0, at, :], wide_keys[tile, 1, at, :]
            total = [before[tile, c, at, :] for c in range(3)]
            for side in sides:
                terms = pair_strength(own, own_key, own_offset, own[6], own[7], *side)
                total = [a + b for a, b in zip(total, terms)]
            for c in range(3):
                forces[tile, c, at, :] = total[c]

    def tile_pairs(tile, carry):
        y = tile % out_y
        blocks = limits[0, tile]
        heights = list(range(slots // 2, slots + 1, STEP))

        def at_height(height):
            def run():
                pair_blocks(tile, y, (0, 1), height, own_forces)

                def one(block, carry):
                    pair_blocks(tile, y, (block,), height, forces)
                    return carry

                lax.fori_loop(2, blocks, one, 0)

            return run

        which = jnp.clip((limits[1, tile] + STEP - 1) // STEP - heights[0] // STEP, 0, len(heights) - 1)
        lax.switch(which, [at_height(h) for h in heights])
        return carry

    ones = jnp.ones((2 * slots, slots), jnp.bfloat16)
    wide_lane = lax.broadcasted_iota(jnp.int32, (slots, slots), 1)
    for zz in range(out_z):
        z = gz * out_z + zz
        total = place_candidates(z)
        present = rows(0, 0, z, 0) < 0.5 * FAR
        blocks = jnp.maximum(1, (total.astype(jnp.int32) + (slots - 1)) >> lane_bits)
        count = jnp.sum(jnp.where(present, 1.0, 0.0), axis=1, keepdims=True).astype(jnp.int32)
        for y in range(out_y):
            limits[0, zz * out_y + y] = blocks[y, 0]
            limits[1, zz * out_y + y] = count[y, 0]
        lax.fori_loop(0, jnp.maximum(2, jnp.max(blocks)), assemble, 0)
        lax.fori_loop(zz * out_y, (zz + 1) * out_y, tile_pairs, 0)
        total = jnp.zeros((slots, slots), jnp.float32)
        for y in range(out_y):
            for c in range(3):
                whole = forces[zz * out_y + y, c]
                if c < 2:
                    sums = jnp.sum(whole, axis=1, keepdims=True)
                else:
                    high = whole.astype(jnp.bfloat16)
                    low = (whole - high.astype(jnp.float32)).astype(jnp.bfloat16)
                    sums = jnp.dot(jnp.concatenate([high, low], axis=1), ones, preferred_element_type=jnp.float32)
                total = jnp.where(wide_lane == c * out_y + y, sums, total)
        kicks = jnp.transpose(total)
        for c in range(3):
            kick = jnp.where(present, kick_scale * UNIT * kicks[c * out_y : (c + 1) * out_y], 0.0)
            for y in range(out_y):
                out_ref[c, 0, y, pl.ds(zz, 1), :] = kick[y : y + 1]


def on_device(nx, ny, nz, positions, velocities, bead_keys, counts):
    _, _, block_y, tiles_z, slots = positions.shape
    out_y, out_z = block_y * nz, tiles_z // nz
    span = out_y + 2
    tiles = out_y * out_z
    gathered = pl.pallas_call(
        functools.partial(gather_kernel, (nx, ny, nz, block_y, tiles_z)),
        out_shape=[
            jax.ShapeDtypeStruct((3, span, tiles_z, ROWS, slots), jnp.float32),
            jax.ShapeDtypeStruct((tiles, 8, slots, slots), jnp.float32),
            jax.ShapeDtypeStruct((tiles, 2, slots, slots), jnp.int32),
            jax.ShapeDtypeStruct((tiles, 3, slots, slots), jnp.float32),
            jax.ShapeDtypeStruct((slots, 5 * slots), jnp.bfloat16),
        ],
        in_specs=[pl.BlockSpec(memory_space=pltpu.HBM)] * 4,
        out_specs=[pl.BlockSpec(memory_space=pltpu.VMEM)] * 5,
        scratch_shapes=[
            pltpu.VMEM(positions.shape, jnp.float32),
            pltpu.VMEM(velocities.shape, jnp.float32),
            pltpu.VMEM(bead_keys.shape, jnp.int32),
            pltpu.SMEM((1, tiles_z, block_y), jnp.int32),
            pltpu.VMEM((block_y, tiles_z, ROWS, slots), jnp.float32),
            pltpu.VMEM((3 * ROWS, ROWS * slots), jnp.bfloat16),
            pltpu.SemaphoreType.DMA((3, nz)),
            pltpu.SemaphoreType.DMA((3, nz)),
            pltpu.SemaphoreType.DMA((2, 3, nz)),
            pltpu.SemaphoreType.DMA((2, 3)),
            pltpu.SemaphoreType.DMA,
            pltpu.SemaphoreType.DMA((4,)),
        ],
        compiler_params=pltpu.CompilerParams(
            collective_id=0, has_side_effects=True, vmem_limit_bytes=12582912
        ),
        name="gather_tiles",
    )(*(pltpu.with_memory_space_constraint(a, pltpu.HBM) for a in (positions, velocities, bead_keys, jnp.swapaxes(counts, 1, 2))))
    shells = len(shell_of(tiles_z))
    return pl.pallas_call(
        functools.partial(pair_kernel, (tiles_z, block_y, out_y, out_z)),
        out_shape=jax.ShapeDtypeStruct((3, 1, out_y, out_z, slots), jnp.float32),
        in_specs=[pl.BlockSpec(memory_space=pltpu.VMEM)] * 5,
        out_specs=pl.BlockSpec(memory_space=pltpu.VMEM),
        scratch_shapes=[
            pltpu.VMEM((shells * out_y, slots), jnp.float32),
            pltpu.VMEM((shells, out_y, slots), jnp.int32),
            pltpu.VMEM((shells, 6, out_y, slots), jnp.float32),
            pltpu.VMEM((shells, out_y, slots), jnp.int32),
            pltpu.VMEM((shells, 7, out_y, slots), jnp.float32),
            pltpu.VMEM((shells, 2, out_y, slots), jnp.int32),
            pltpu.VMEM((tiles, 3, slots, slots), jnp.float32),
            pltpu.SMEM((2, tiles), jnp.int32),
        ],
        compiler_params=pltpu.CompilerParams(vmem_limit_bytes=16777216),
        name="pair_kicks",
    )(*gathered)


def solution(mesh):
    in_specs = (
        P(None, "gx", ("gy", "gz"), None, None),
        P(None, "gx", ("gy", "gz"), None, None),
        P("gx", ("gy", "gz"), None, None),
        P("gx", ("gy", "gz"), None),
    )
    out_specs = P(None, "gx", "gy", "gz", None)
    nx, ny, nz = mesh.shape["gx"], mesh.shape["gy"], mesh.shape["gz"]
    return jax.shard_map(
        functools.partial(on_device, nx, ny, nz),
        mesh=mesh,
        in_specs=in_specs,
        out_specs=out_specs,
        check_vma=False,
    )
```

```python
import functools

import jax
import jax.numpy as jnp
from jax import lax
from jax.experimental import pallas as pl
from jax.experimental.pallas import tpu as pltpu
from jax.sharding import PartitionSpec as P

SIDE = 3.0

soft_radius = 0.05
friction = 4.5
noise_amplitude = 15.0
like_repulsion = 25.0
unlike_extra = 15.0
kick_scale = 0.02
root_twelve = 3.4641016151377544

FAR = 1.0e9
ROWS = 8
KEY_A = 1103515245
KEY_B = 12345
KEY_C = 747796405
STEP = 16
REACH = 1.00001
UNIT = noise_amplitude * root_twelve / 2147483648.0
MESH = pl.DeviceIdType.MESH


def pair_strength(own, own_key, own_offset, own_even, own_odd, other, key, offset, even):
    sep = [own[c] - other[c] for c in range(3)]
    squared = sep[0] * sep[0] + sep[1] * sep[1] + sep[2] * sep[2]
    root = lax.rsqrt(jnp.maximum(squared, 1e-30))
    scaled = jnp.maximum(1.0 - squared * root, 0.0) * jnp.minimum(root, 1.0 / soft_radius)
    dot = sep[0] * (own[3] - other[3]) + sep[1] * (own[4] - other[4]) + sep[2] * (own[5] - other[5])
    hashed = (own_key ^ key) * KEY_A + (own_offset + offset)
    hashed = hashed ^ lax.shift_right_logical(hashed, 15)
    hashed = hashed * KEY_C
    hashed = hashed ^ lax.shift_right_logical(hashed, 13)
    push = (hashed & 0x7FFFFF80).astype(jnp.float32) + jnp.where(even, own_even, own_odd)
    strength = scaled * (push - scaled * dot)
    return [strength * part for part in sep]


def split(values):
    high = values.astype(jnp.bfloat16).astype(jnp.float32)
    middle = (values - high).astype(jnp.bfloat16).astype(jnp.float32)
    return [high, middle, values - high - middle]


def column_of(tiles_z):
    return [None] if tiles_z == 2 else [-1, 1]


def own_tile(tile, brick, y, z, paired, select, wide, wide_keys, forces):
    tiles_z, block_y, _, slots = brick.shape
    rows = brick[z, y]
    parts = split(rows)
    spread = jnp.dot(jnp.transpose(jnp.concatenate(parts, axis=0)).astype(jnp.bfloat16), select[...], preferred_element_type=jnp.float32)

    def side(near, dz, shift_y=None):
        motion = [near[c : c + 1] for c in range(6)]
        if dz is None:
            motion[2] = motion[2] + jnp.where(motion[2] < 0.5 * SIDE, SIDE, -SIDE)
        elif dz:
            motion[2] = motion[2] + SIDE * dz
        if shift_y is not None:
            motion[1] = motion[1] + shift_y
        key = near[6:7].astype(jnp.int32) * 32768 + near[7:8].astype(jnp.int32)
        motion, key = [jnp.broadcast_to(m, (8, slots)) for m in motion], jnp.broadcast_to(key, (8, slots))
        return motion, key, key * KEY_B, (key & 1) == 0

    sides = [side(rows, 0)]
    for dz in column_of(tiles_z):
        sides.append(side(brick[1 - z if dz is None else lax.rem(z + dz + tiles_z, tiles_z), y], dz))
    if paired and block_y > 1:
        step = 1 - 2 * (y // (block_y // 2))
        sides.append(side(brick[z, y + step], 0, step.astype(jnp.float32) * SIDE))
    level = (like_repulsion - 0.5 * noise_amplitude * root_twelve) / UNIT
    for g in range(0, slots, 8):
        at = pl.ds(g, 8)
        part = [spread[g : g + 8, c * slots : (c + 1) * slots] for c in range(8)]
        low = part[7].astype(jnp.int32)
        own_key = part[6].astype(jnp.int32) * 32768 + low
        own_offset = own_key * KEY_B
        kind = (low & 1).astype(jnp.float32) * (unlike_extra / UNIT)
        own_even = level + kind
        own_odd = (level + unlike_extra / UNIT) - kind
        for c in range(6):
            wide[tile, c, at, :] = part[c]
        wide[tile, 6, at, :] = own_even
        wide[tile, 7, at, :] = own_odd
        wide_keys[tile, 0, at, :] = own_key
        wide_keys[tile, 1, at, :] = own_offset
        terms = [pair_strength(part, own_key, own_offset, own_even, own_odd, *one) for one in sides]
        for c in range(3):
            forces[tile, c, at, :] = functools.reduce(jnp.add, [term[c] for term in terms])


def gather_kernel(sizes, pos_in, vel_in, key_in, count_in, all_ref, wide, wide_keys, forces, below, pos_ref, vel_ref, key_ref, count_ref, packed, select, send, recv, edge_send, edge_recv, local, loads):
    nx, ny, nz, block_y, tiles_z = sizes
    gx, gy, gz = lax.axis_index("gx"), lax.axis_index("gy"), lax.axis_index("gz")
    slots = pos_ref.shape[-1]
    inputs = ((pos_in, pos_ref), (vel_in, vel_ref), (key_in, key_ref), (count_in, count_ref))
    fetches = [pltpu.make_async_copy(a, b, loads.at[k]) for k, (a, b) in enumerate(inputs)]
    for fetch in fetches:
        fetch.start()
    top = nz * block_y + 1
    barrier = pltpu.get_barrier_semaphore()

    def target(e, group, member):
        return (lax.rem(gx + e + nx, nx), lax.rem(gy + group + ny, ny), lax.rem(member + nz, nz))

    steps = (-1, 0, 1)
    for e in (-1, 1, 0):
        pl.semaphore_signal(barrier, inc=1, device_id=target(e, -1, nz - 1), device_id_type=MESH)
        pl.semaphore_signal(barrier, inc=1, device_id=target(e, 1, 0), device_id_type=MESH)
    for r in reversed(range(nz)):
        for e in (-1, 1, 0):
            if e or r:
                pl.semaphore_signal(barrier, inc=1, device_id=target(e, 0, gz + r), device_id_type=MESH)

    row = lax.broadcasted_iota(jnp.int32, select.shape, 0)
    column = lax.broadcasted_iota(jnp.int32, select.shape, 1)
    chosen = (row & (ROWS - 1)) == (column >> (slots - 1).bit_length())
    select[...] = jnp.where(chosen, 1.0, 0.0).astype(jnp.bfloat16)
    lane_bits = (slots - 1).bit_length()
    row = lax.broadcasted_iota(jnp.int32, below.shape, 0)
    column = lax.broadcasted_iota(jnp.int32, below.shape, 1)
    limit = jnp.where(column < slots, column + 1, (column >> lane_bits) * (slots // 8))
    below[...] = jnp.where(row < limit, 1.0, 0.0).astype(jnp.bfloat16)
    for fetch in fetches:
        fetch.wait()
    lane = lax.broadcasted_iota(jnp.int32, (1, slots), 1)
    for y in range(block_y):
        for z in range(tiles_z):
            present = lane < count_ref[0, z, y]
            key = key_ref[0, y, pl.ds(z, 1), :]
            rows = [jnp.where(present, pos_ref[c, 0, y, pl.ds(z, 1), :], FAR) for c in range(3)]
            rows += [vel_ref[c, 0, y, pl.ds(z, 1), :] * (friction / UNIT) for c in range(3)]
            rows += [(key >> 15).astype(jnp.float32), (key & 32767).astype(jnp.float32)]
            packed[z, y] = jnp.concatenate(rows, axis=0)

    def group_copy(e, r, slot_of):
        return pltpu.make_async_remote_copy(
            src_ref=packed,
            dst_ref=all_ref.at[1 - e, :, pl.ds(1 + slot_of * block_y, block_y)],
            send_sem=send.at[e + 1, r],
            recv_sem=recv.at[e + 1, r],
            device_id=target(e, 0, gz + r),
            device_id_type=MESH,
        )

    def edge_copy(e, side, member):
        first = side == 0
        return pltpu.make_async_remote_copy(
            src_ref=packed.at[:, pl.ds(0 if first else block_y - 1, 1)],
            dst_ref=all_ref.at[1 - e, :, pl.ds(top if first else 0, 1)],
            send_sem=edge_send.at[side, e + 1, member],
            recv_sem=edge_recv.at[side, e + 1],
            device_id=target(e, -1 if first else 1, member),
            device_id_type=MESH,
        )

    ends = jnp.where(gz == 0, 1, 0) + jnp.where(gz == nz - 1, 1, 0)
    pl.semaphore_wait(barrier, 3 * nz - 1 + 3 * nz * ends)

    def edges(side, act):
        for e in (-1, 1, 0):
            for member in range(nz):
                act(edge_copy(e, side, member))

    @pl.when(gz == 0)
    def _():
        edges(0, lambda c: c.start())

    @pl.when(gz == nz - 1)
    def _():
        edges(1, lambda c: c.start())

    for r in reversed(range(nz)):
        for e in (0, -1, 1):
            if e or r:
                group_copy(e, r, gz).start()

    mine = pltpu.make_async_copy(packed, all_ref.at[1, :, pl.ds(1 + gz * block_y, block_y)], local)
    mine.start()
    out_y, out_z = nz * block_y, tiles_z // nz
    for zz in range(out_z):

        def near_one(y, carry, zz=zz):
            own_tile(zz * out_y + gz * block_y + y, packed, y, gz * out_z + zz, True, select, wide, wide_keys, forces)
            return carry

        lax.fori_loop(0, block_y, near_one, 0, unroll=min(2, block_y))

    for r in range(1, nz):
        slot_of = lax.rem(gz - r + nz, nz)
        group_copy(0, r, slot_of).wait_recv()
        for zz in range(out_z):

            def remote(y, carry, zz=zz, slot_of=slot_of):
                at = slot_of * block_y + y
                own_tile(zz * out_y + at, all_ref.at[1, :, pl.ds(1 + slot_of * block_y, block_y)], y, gz * out_z + zz, False, select, wide, wide_keys, forces)
                return carry

            lax.fori_loop(0, block_y, remote, 0, unroll=min(2, block_y))

    mine.wait()
    for e in steps:
        for r in range(nz):
            if e or r:
                copy = group_copy(e, r, lax.rem(gz - r + nz, nz))
                if e:
                    copy.wait_recv()
                copy.wait_send()
        for side in range(2):
            edge_copy(e, side, 0).wait_recv()

    @pl.when(gz == 0)
    def _():
        edges(0, lambda c: c.wait_send())

    @pl.when(gz == nz - 1)
    def _():
        edges(1, lambda c: c.wait_send())


def shell_of(tiles_z):
    layers = (0, None) if tiles_z == 2 else (-1, 0, 1)
    offsets = [(dx, dy, dz) for dx in (-1, 0, 1) for dy in (-1, 0, 1) for dz in layers]
    done = [(0, 0, dz) for dz in [0] + column_of(tiles_z)]
    return [offset for offset in offsets if offset not in done]


def pair_kernel(sizes, all_ref, wide, wide_keys, own_forces, below, out_ref, masks, places, moved, moved_keys, near, near_keys, forces, limits):
    tiles_z, block_y, out_y, out_z = sizes
    slots = all_ref.shape[-1]
    span = all_ref.shape[2]
    gz = lax.axis_index("gz")
    shell = shell_of(tiles_z)
    n = len(shell)
    lane_bits = (slots - 1).bit_length()
    eighth = slots // 8
    flat = all_ref.reshape(3 * span * tiles_z * ROWS, slots)
    lane = lax.broadcasted_iota(jnp.int32, (out_y, slots), 1)
    line = lax.broadcasted_iota(jnp.int32, (out_y, slots), 0)

    def rows(dx, dy, z, c):
        start = (((1 + dx) * tiles_z + z) * span + 1 + dy) * ROWS + c
        return flat[pl.ds(start, out_y, stride=ROWS), :]

    def keys_of(dx, dy, z):
        return rows(dx, dy, z, 6).astype(jnp.int32) * 32768 + rows(dx, dy, z, 7).astype(jnp.int32)

    def empty():
        motion = [jnp.full((out_y, slots), FAR if c < 3 else 0.0, jnp.float32) for c in range(6)]
        return motion, jnp.zeros((out_y, slots), jnp.int32)

    def place_candidates(z):
        def position(k):
            dx, dy, dz = shell[k]
            other = 1 - z if dz is None else lax.rem(z + dz + tiles_z, tiles_z)
            p = [rows(dx, dy, other, c) for c in range(3)]
            if dx:
                p[0] = p[0] + SIDE * dx
            if dy:
                p[1] = p[1] + SIDE * dy
            if dz is None:
                p[2] = p[2] + jnp.where(p[2] < 0.5 * SIDE, SIDE, -SIDE)
            elif dz:
                p[2] = p[2] + SIDE * dz
            return p, other

        for k in range(n):
            dx, dy, dz = shell[k]
            other = 1 - z if dz is None else lax.rem(z + dz + tiles_z, tiles_z)
            gap = None
            for c, side in enumerate((dx, dy, dz)):
                if side != 0:
                    value = rows(dx, dy, other, c)
                    if side is None:
                        value = jnp.minimum(value, SIDE - value)
                    elif side < 0:
                        value = SIDE - value
                    gap = value * value if gap is None else gap + value * value
            inside = gap < REACH
            if dx == 0 and dz == 0 and block_y > 1:
                step = 1 - 2 * ((line % block_y) // (block_y // 2))
                inside = inside & ((step != dy) | (line < gz * block_y) | (line >= (gz + 1) * block_y))
            masks[pl.ds(k * out_y, out_y), :] = jnp.where(inside, 1.0, 0.0)

        sums = jnp.dot(masks[...].astype(jnp.bfloat16), below[...], preferred_element_type=jnp.float32)
        start = jnp.zeros((out_y, slots), jnp.float32)
        ready = [empty(), empty()]
        seek = []
        for k in range(n):
            part = [sums[k * out_y : (k + 1) * out_y, q * slots : (q + 1) * slots] for q in range(9)]
            first = start.astype(jnp.int32)
            want = (lane - first) & (slots - 1)
            level = want.astype(jnp.float32)
            upper = part[4] <= level
            second = jnp.where(upper, part[6], part[2]) <= level
            third = jnp.where(second, jnp.where(upper, part[7], part[3]), jnp.where(upper, part[5], part[1])) <= level
            at = jnp.where(upper, 4 * eighth, 0) + jnp.where(second, 2 * eighth, 0) + jnp.where(third, eighth, 0)
            place = jnp.where(level < part[8], (first + want) >> lane_bits, -1)
            places[k] = place
            seek.append((part[0], level, at, place))
            start = start + part[8]
        bit = eighth // 2
        while bit:
            for k, (before, level, at, place) in enumerate(seek):
                seen = jnp.take_along_axis(before, at + (bit - 1), axis=1, mode="promise_in_bounds")
                seek[k] = before, level, jnp.where(seen <= level, at + bit, at), place
            bit //= 2
        for k in range(n):
            _, _, at, place = seek[k]
            p, other = position(k)
            dx, dy, _ = shell[k]
            p += [rows(dx, dy, other, c) for c in range(3, 6)]
            for c in range(6):
                moved[k, c] = jnp.take_along_axis(p[c], at, axis=1, mode="promise_in_bounds")
            moved_keys[k] = jnp.take_along_axis(keys_of(dx, dy, other), at, axis=1, mode="promise_in_bounds")
            for block in range(2):
                here = place == block
                motion, key = ready[block]
                motion = [jnp.where(here, moved[k, c], motion[c]) for c in range(6)]
                ready[block] = motion, jnp.where(here, moved_keys[k], key)
        for block in range(2):
            keep(block, *ready[block])
        return start

    def keep(block, motion, key):
        for c in range(6):
            near[block, c] = motion[c]
        near[block, 6] = (key & 1).astype(jnp.float32)
        near_keys[block, 0] = key
        near_keys[block, 1] = key * KEY_B

    def assemble(block, carry):
        motion, key = empty()
        for k in range(n):
            here = places[k] == block
            motion = [jnp.where(here, moved[k, c], motion[c]) for c in range(6)]
            key = jnp.where(here, moved_keys[k], key)
        keep(block, motion, key)
        return carry

    def pair_blocks(tile, y, blocks, height, before):
        sides = []
        for block in blocks:
            other = [jnp.broadcast_to(near[block, c, pl.ds(y, 1), :], (8, slots)) for c in range(7)]
            key = jnp.broadcast_to(near_keys[block, 0, pl.ds(y, 1), :], (8, slots))
            offset = jnp.broadcast_to(near_keys[block, 1, pl.ds(y, 1), :], (8, slots))
            sides.append((other, key, offset, other[6] < 0.5))
        for g in range(0, height, 8):
            at = pl.ds(g, 8)
            own = [wide[tile, c, at, :] for c in range(8)]
            own_key, own_offset = wide_keys[tile, 0, at, :], wide_keys[tile, 1, at, :]
            total = [before[tile, c, at, :] for c in range(3)]
            for side in sides:
                terms = pair_strength(own, own_key, own_offset, own[6], own[7], *side)
                total = [a + b for a, b in zip(total, terms)]
            for c in range(3):
                forces[tile, c, at, :] = total[c]

    heights = list(range(slots // 2, slots + 1, STEP))

    def tile_pairs(zz, y, carry):
        tile = zz * out_y + y

        def at_height(height):
            def run():
                pair_blocks(tile, y, (0, 1), height, own_forces)

                def one(block, carry):
                    pair_blocks(tile, y, (block,), height, forces)
                    return carry

                lax.fori_loop(2, limits[0, tile], one, 0)

            return run

        lax.switch(limits[1, tile], [at_height(h) for h in heights])
        return carry

    ones = jnp.ones((2 * slots, slots), jnp.bfloat16)
    wide_lane = lax.broadcasted_iota(jnp.int32, (slots, slots), 1)
    for zz in range(out_z):
        z = gz * out_z + zz
        total = place_candidates(z)
        present = rows(0, 0, z, 0) < 0.5 * FAR
        blocks = jnp.maximum(1, (total.astype(jnp.int32) + (slots - 1)) >> lane_bits)
        count = jnp.sum(jnp.where(present, 1.0, 0.0), axis=1, keepdims=True).astype(jnp.int32)
        which = jnp.maximum((count + (STEP - 1)) // STEP - heights[0] // STEP, 0)
        for y in range(out_y):
            limits[0, zz * out_y + y] = blocks[y, 0]
            limits[1, zz * out_y + y] = which[y, 0]
        lax.fori_loop(2, jnp.max(blocks), assemble, 0)
        lax.fori_loop(0, out_y, functools.partial(tile_pairs, zz), 0)
        total = jnp.zeros((slots, slots), jnp.float32)
        for y in range(out_y):
            for c in range(3):
                whole = forces[zz * out_y + y, c]
                if c < 2:
                    sums = jnp.sum(whole, axis=1, keepdims=True)
                else:
                    high = whole.astype(jnp.bfloat16)
                    low = (whole - high.astype(jnp.float32)).astype(jnp.bfloat16)
                    sums = jnp.dot(jnp.concatenate([high, low], axis=1), ones, preferred_element_type=jnp.float32)
                total = jnp.where(wide_lane == c * out_y + y, sums, total)
        kicks = jnp.transpose(total)
        for c in range(3):
            kick = jnp.where(present, kick_scale * UNIT * kicks[c * out_y : (c + 1) * out_y], 0.0)
            for y in range(out_y):
                out_ref[c, 0, y, pl.ds(zz, 1), :] = kick[y : y + 1]


def on_device(nx, ny, nz, positions, velocities, bead_keys, counts):
    _, _, block_y, tiles_z, slots = positions.shape
    out_y, out_z = block_y * nz, tiles_z // nz
    span = out_y + 2
    tiles = out_y * out_z
    gathered = pl.pallas_call(
        functools.partial(gather_kernel, (nx, ny, nz, block_y, tiles_z)),
        out_shape=[
            jax.ShapeDtypeStruct((3, tiles_z, span, ROWS, slots), jnp.float32),
            jax.ShapeDtypeStruct((tiles, 8, slots, slots), jnp.float32),
            jax.ShapeDtypeStruct((tiles, 2, slots, slots), jnp.int32),
            jax.ShapeDtypeStruct((tiles, 3, slots, slots), jnp.float32),
            jax.ShapeDtypeStruct((slots, 9 * slots), jnp.bfloat16),
        ],
        in_specs=[pl.BlockSpec(memory_space=pltpu.HBM)] * 4,
        out_specs=[pl.BlockSpec(memory_space=pltpu.VMEM)] * 5,
        scratch_shapes=[
            pltpu.VMEM(positions.shape, jnp.float32),
            pltpu.VMEM(velocities.shape, jnp.float32),
            pltpu.VMEM(bead_keys.shape, jnp.int32),
            pltpu.SMEM((1, tiles_z, block_y), jnp.int32),
            pltpu.VMEM((tiles_z, block_y, ROWS, slots), jnp.float32),
            pltpu.VMEM((3 * ROWS, ROWS * slots), jnp.bfloat16),
            pltpu.SemaphoreType.DMA((3, nz)),
            pltpu.SemaphoreType.DMA((3, nz)),
            pltpu.SemaphoreType.DMA((2, 3, nz)),
            pltpu.SemaphoreType.DMA((2, 3)),
            pltpu.SemaphoreType.DMA,
            pltpu.SemaphoreType.DMA((4,)),
        ],
        compiler_params=pltpu.CompilerParams(
            collective_id=0, has_side_effects=True, vmem_limit_bytes=12582912
        ),
        name="gather_tiles",
    )(*(pltpu.with_memory_space_constraint(a, pltpu.HBM) for a in (positions, velocities, bead_keys, jnp.swapaxes(counts, 1, 2))))
    shells = len(shell_of(tiles_z))
    return pl.pallas_call(
        functools.partial(pair_kernel, (tiles_z, block_y, out_y, out_z)),
        out_shape=jax.ShapeDtypeStruct((3, 1, out_y, out_z, slots), jnp.float32),
        in_specs=[pl.BlockSpec(memory_space=pltpu.VMEM)] * 5,
        out_specs=pl.BlockSpec(memory_space=pltpu.VMEM),
        scratch_shapes=[
            pltpu.VMEM((shells * out_y, slots), jnp.float32),
            pltpu.VMEM((shells, out_y, slots), jnp.int32),
            pltpu.VMEM((shells, 6, out_y, slots), jnp.float32),
            pltpu.VMEM((shells, out_y, slots), jnp.int32),
            pltpu.VMEM((shells, 7, out_y, slots), jnp.float32),
            pltpu.VMEM((shells, 2, out_y, slots), jnp.int32),
            pltpu.VMEM((tiles, 3, slots, slots), jnp.float32),
            pltpu.SMEM((2, tiles), jnp.int32),
        ],
        compiler_params=pltpu.CompilerParams(vmem_limit_bytes=16777216),
        name="pair_kicks",
    )(*gathered)


def solution(mesh):
    in_specs = (
        P(None, "gx", ("gy", "gz"), None, None),
        P(None, "gx", ("gy", "gz"), None, None),
        P("gx", ("gy", "gz"), None, None),
        P("gx", ("gy", "gz"), None),
    )
    out_specs = P(None, "gx", "gy", "gz", None)
    nx, ny, nz = mesh.shape["gx"], mesh.shape["gy"], mesh.shape["gz"]
    return jax.shard_map(
        functools.partial(on_device, nx, ny, nz),
        mesh=mesh,
        in_specs=in_specs,
        out_specs=out_specs,
        check_vma=False,
    )
```

```python
import functools

import jax
import jax.numpy as jnp
from jax import lax
from jax.experimental import pallas as pl
from jax.experimental.pallas import tpu as pltpu
from jax.sharding import PartitionSpec as P

SIDE = 3.0

soft_radius = 0.05
friction = 4.5
noise_amplitude = 15.0
like_repulsion = 25.0
unlike_extra = 15.0
kick_scale = 0.02
root_twelve = 3.4641016151377544

FAR = 1.0e9
ROWS = 8
KEY_A = 1103515245
KEY_B = 12345
KEY_C = 747796405
STEP = 16
REACH = 1.00001
UNIT = noise_amplitude * root_twelve / 2147483648.0
MESH = pl.DeviceIdType.MESH


def pair_strength(own, own_key, own_offset, own_even, own_odd, other, key, offset, even):
    sep = [own[c] - other[c] for c in range(3)]
    squared = sep[0] * sep[0] + sep[1] * sep[1] + sep[2] * sep[2]
    root = lax.rsqrt(jnp.maximum(squared, 1e-30))
    scaled = jnp.maximum(1.0 - squared * root, 0.0) * jnp.minimum(root, 1.0 / soft_radius)
    dot = sep[0] * (own[3] - other[3]) + sep[1] * (own[4] - other[4]) + sep[2] * (own[5] - other[5])
    hashed = (own_key ^ key) * KEY_A + (own_offset + offset)
    hashed = hashed ^ lax.shift_right_logical(hashed, 15)
    hashed = hashed * KEY_C
    hashed = hashed ^ lax.shift_right_logical(hashed, 13)
    push = (hashed & 0x7FFFFF80).astype(jnp.float32) + jnp.where(even, own_even, own_odd)
    strength = scaled * (push - scaled * dot)
    return [strength * part for part in sep]


def split(values):
    high = values.astype(jnp.bfloat16).astype(jnp.float32)
    middle = (values - high).astype(jnp.bfloat16).astype(jnp.float32)
    return [high, middle, values - high - middle]


def column_of(tiles_z):
    return [None] if tiles_z == 2 else [-1, 1]


def own_tile(tile, brick, y, z, paired, select, wide, wide_keys, forces):
    tiles_z, block_y, _, slots = brick.shape
    rows = brick[z, y]
    parts = split(rows)
    spread = jnp.dot(jnp.transpose(jnp.concatenate(parts, axis=0)).astype(jnp.bfloat16), select[...], preferred_element_type=jnp.float32)

    def side(near, dz, shift_y=None):
        motion = [near[c : c + 1] for c in range(6)]
        if dz is None:
            motion[2] = motion[2] + jnp.where(motion[2] < 0.5 * SIDE, SIDE, -SIDE)
        elif dz:
            motion[2] = motion[2] + SIDE * dz
        if shift_y is not None:
            motion[1] = motion[1] + shift_y
        key = near[6:7].astype(jnp.int32) * 32768 + near[7:8].astype(jnp.int32)
        motion, key = [jnp.broadcast_to(m, (8, slots)) for m in motion], jnp.broadcast_to(key, (8, slots))
        return motion, key, key * KEY_B, (key & 1) == 0

    sides = [side(rows, 0)]
    for dz in column_of(tiles_z):
        sides.append(side(brick[1 - z if dz is None else lax.rem(z + dz + tiles_z, tiles_z), y], dz))
    if paired and block_y > 1:
        step = 1 - 2 * (y // (block_y // 2))
        sides.append(side(brick[z, y + step], 0, step.astype(jnp.float32) * SIDE))
    level = (like_repulsion - 0.5 * noise_amplitude * root_twelve) / UNIT
    for g in range(0, slots, 8):
        at = pl.ds(g, 8)
        part = [spread[g : g + 8, c * slots : (c + 1) * slots] for c in range(8)]
        low = part[7].astype(jnp.int32)
        own_key = part[6].astype(jnp.int32) * 32768 + low
        own_offset = own_key * KEY_B
        kind = (low & 1).astype(jnp.float32) * (unlike_extra / UNIT)
        own_even = level + kind
        own_odd = (level + unlike_extra / UNIT) - kind
        for c in range(6):
            wide[tile, c, at, :] = part[c]
        wide[tile, 6, at, :] = own_even
        wide[tile, 7, at, :] = own_odd
        wide_keys[tile, 0, at, :] = own_key
        wide_keys[tile, 1, at, :] = own_offset
        terms = [pair_strength(part, own_key, own_offset, own_even, own_odd, *one) for one in sides]
        for c in range(3):
            forces[tile, c, at, :] = functools.reduce(jnp.add, [term[c] for term in terms])


def gather_kernel(sizes, pos_in, vel_in, key_in, count_in, all_ref, wide, wide_keys, forces, below, pos_ref, vel_ref, key_ref, count_ref, packed, select, send, recv, edge_send, edge_recv, local, loads):
    nx, ny, nz, block_y, tiles_z = sizes
    gx, gy, gz = lax.axis_index("gx"), lax.axis_index("gy"), lax.axis_index("gz")
    slots = pos_ref.shape[-1]
    inputs = ((pos_in, pos_ref), (vel_in, vel_ref), (key_in, key_ref), (count_in, count_ref))
    fetches = [pltpu.make_async_copy(a, b, loads.at[k]) for k, (a, b) in enumerate(inputs)]
    for fetch in fetches:
        fetch.start()
    top = nz * block_y + 1
    barrier = pltpu.get_barrier_semaphore()

    def target(e, group, member):
        return (lax.rem(gx + e + nx, nx), lax.rem(gy + group + ny, ny), lax.rem(member + nz, nz))

    steps = (-1, 0, 1)
    for e in (-1, 1, 0):
        pl.semaphore_signal(barrier, inc=1, device_id=target(e, -1, nz - 1), device_id_type=MESH)
        pl.semaphore_signal(barrier, inc=1, device_id=target(e, 1, 0), device_id_type=MESH)
    for r in reversed(range(nz)):
        for e in (-1, 1, 0):
            if e or r:
                pl.semaphore_signal(barrier, inc=1, device_id=target(e, 0, gz + r), device_id_type=MESH)

    row = lax.broadcasted_iota(jnp.int32, select.shape, 0)
    column = lax.broadcasted_iota(jnp.int32, select.shape, 1)
    chosen = (row & (ROWS - 1)) == (column >> (slots - 1).bit_length())
    select[...] = jnp.where(chosen, 1.0, 0.0).astype(jnp.bfloat16)
    lane_bits = (slots - 1).bit_length()
    row = lax.broadcasted_iota(jnp.int32, below.shape, 0)
    column = lax.broadcasted_iota(jnp.int32, below.shape, 1)
    limit = jnp.where(column < slots, column + 1, (column >> lane_bits) * (slots // 8))
    below[...] = jnp.where(row < limit, 1.0, 0.0).astype(jnp.bfloat16)
    for fetch in fetches:
        fetch.wait()
    lane = lax.broadcasted_iota(jnp.int32, (1, slots), 1)
    for y in range(block_y):
        for z in range(tiles_z):
            present = lane < count_ref[0, z, y]
            key = key_ref[0, y, pl.ds(z, 1), :]
            rows = [jnp.where(present, pos_ref[c, 0, y, pl.ds(z, 1), :], FAR) for c in range(3)]
            rows += [vel_ref[c, 0, y, pl.ds(z, 1), :] * (friction / UNIT) for c in range(3)]
            rows += [(key >> 15).astype(jnp.float32), (key & 32767).astype(jnp.float32)]
            packed[z, y] = jnp.concatenate(rows, axis=0)

    def group_copy(e, r, slot_of):
        return pltpu.make_async_remote_copy(
            src_ref=packed,
            dst_ref=all_ref.at[1 - e, :, pl.ds(1 + slot_of * block_y, block_y)],
            send_sem=send.at[e + 1, r],
            recv_sem=recv.at[e + 1, r],
            device_id=target(e, 0, gz + r),
            device_id_type=MESH,
        )

    def edge_copy(e, side, member):
        first = side == 0
        return pltpu.make_async_remote_copy(
            src_ref=packed.at[:, pl.ds(0 if first else block_y - 1, 1)],
            dst_ref=all_ref.at[1 - e, :, pl.ds(top if first else 0, 1)],
            send_sem=edge_send.at[side, e + 1, member],
            recv_sem=edge_recv.at[side, e + 1],
            device_id=target(e, -1 if first else 1, member),
            device_id_type=MESH,
        )

    ends = jnp.where(gz == 0, 1, 0) + jnp.where(gz == nz - 1, 1, 0)
    pl.semaphore_wait(barrier, 3 * nz - 1 + 3 * nz * ends)

    def edges(side, act):
        for e in (-1, 1, 0):
            for member in range(nz):
                act(edge_copy(e, side, member))

    @pl.when(gz == 0)
    def _():
        edges(0, lambda c: c.start())

    @pl.when(gz == nz - 1)
    def _():
        edges(1, lambda c: c.start())

    for r in reversed(range(nz)):
        for e in (0, -1, 1):
            if e or r:
                group_copy(e, r, gz).start()

    mine = pltpu.make_async_copy(packed, all_ref.at[1, :, pl.ds(1 + gz * block_y, block_y)], local)
    mine.start()
    out_y, out_z = nz * block_y, tiles_z // nz
    for zz in range(out_z):

        def near_one(y, carry, zz=zz):
            own_tile(zz * out_y + gz * block_y + y, packed, y, gz * out_z + zz, True, select, wide, wide_keys, forces)
            return carry

        lax.fori_loop(0, block_y, near_one, 0, unroll=min(4, block_y))

    for r in range(1, nz):
        slot_of = lax.rem(gz - r + nz, nz)
        group_copy(0, r, slot_of).wait_recv()
        for zz in range(out_z):

            def remote(y, carry, zz=zz, slot_of=slot_of):
                at = slot_of * block_y + y
                own_tile(zz * out_y + at, all_ref.at[1, :, pl.ds(1 + slot_of * block_y, block_y)], y, gz * out_z + zz, True, select, wide, wide_keys, forces)
                return carry

            lax.fori_loop(0, block_y, remote, 0, unroll=min(4, block_y))

    mine.wait()
    for e in steps:
        for r in range(nz):
            if e or r:
                copy = group_copy(e, r, lax.rem(gz - r + nz, nz))
                if e:
                    copy.wait_recv()
                copy.wait_send()
        for side in range(2):
            edge_copy(e, side, 0).wait_recv()

    @pl.when(gz == 0)
    def _():
        edges(0, lambda c: c.wait_send())

    @pl.when(gz == nz - 1)
    def _():
        edges(1, lambda c: c.wait_send())


def shell_of(tiles_z):
    layers = (0, None) if tiles_z == 2 else (-1, 0, 1)
    offsets = [(dx, dy, dz) for dx in (-1, 0, 1) for dy in (-1, 0, 1) for dz in layers]
    done = [(0, 0, dz) for dz in [0] + column_of(tiles_z)]
    return [offset for offset in offsets if offset not in done]


def pair_kernel(sizes, all_ref, wide, wide_keys, own_forces, below, out_ref, masks, places, moved, moved_keys, near, near_keys, forces, limits):
    tiles_z, block_y, out_y, out_z = sizes
    slots = all_ref.shape[-1]
    span = all_ref.shape[2]
    gz = lax.axis_index("gz")
    shell = shell_of(tiles_z)
    n = len(shell)
    lane_bits = (slots - 1).bit_length()
    eighth = slots // 8
    flat = all_ref.reshape(3 * span * tiles_z * ROWS, slots)
    lane = lax.broadcasted_iota(jnp.int32, (out_y, slots), 1)
    line = lax.broadcasted_iota(jnp.int32, (out_y, slots), 0)

    def rows(dx, dy, z, c):
        start = (((1 + dx) * tiles_z + z) * span + 1 + dy) * ROWS + c
        return flat[pl.ds(start, out_y, stride=ROWS), :]

    def keys_of(dx, dy, z):
        return rows(dx, dy, z, 6).astype(jnp.int32) * 32768 + rows(dx, dy, z, 7).astype(jnp.int32)

    def empty():
        motion = [jnp.full((out_y, slots), FAR if c < 3 else 0.0, jnp.float32) for c in range(6)]
        return motion, jnp.zeros((out_y, slots), jnp.int32)

    def place_candidates(z):
        def position(k):
            dx, dy, dz = shell[k]
            other = 1 - z if dz is None else lax.rem(z + dz + tiles_z, tiles_z)
            p = [rows(dx, dy, other, c) for c in range(3)]
            if dx:
                p[0] = p[0] + SIDE * dx
            if dy:
                p[1] = p[1] + SIDE * dy
            if dz is None:
                p[2] = p[2] + jnp.where(p[2] < 0.5 * SIDE, SIDE, -SIDE)
            elif dz:
                p[2] = p[2] + SIDE * dz
            return p, other

        for k in range(n):
            dx, dy, dz = shell[k]
            other = 1 - z if dz is None else lax.rem(z + dz + tiles_z, tiles_z)
            gap = None
            for c, side in enumerate((dx, dy, dz)):
                if side != 0:
                    value = rows(dx, dy, other, c)
                    if side is None:
                        value = jnp.minimum(value, SIDE - value)
                    elif side < 0:
                        value = SIDE - value
                    gap = value * value if gap is None else gap + value * value
            inside = gap < REACH
            if dx == 0 and dz == 0 and block_y > 1:
                step = 1 - 2 * ((line % block_y) // (block_y // 2))
                inside = inside & (step != dy)
            masks[pl.ds(k * out_y, out_y), :] = jnp.where(inside, 1.0, 0.0)

        sums = jnp.dot(masks[...].astype(jnp.bfloat16), below[...], preferred_element_type=jnp.float32)
        start = jnp.zeros((out_y, slots), jnp.float32)
        ready = [empty(), empty()]
        seek = []
        for k in range(n):
            part = [sums[k * out_y : (k + 1) * out_y, q * slots : (q + 1) * slots] for q in range(9)]
            first = start.astype(jnp.int32)
            want = (lane - first) & (slots - 1)
            level = want.astype(jnp.float32)
            upper = part[4] <= level
            second = jnp.where(upper, part[6], part[2]) <= level
            third = jnp.where(second, jnp.where(upper, part[7], part[3]), jnp.where(upper, part[5], part[1])) <= level
            at = jnp.where(upper, 4 * eighth, 0) + jnp.where(second, 2 * eighth, 0) + jnp.where(third, eighth, 0)
            place = jnp.where(level < part[8], (first + want) >> lane_bits, -1)
            places[k] = place
            seek.append((part[0], level, at, place))
            start = start + part[8]
        bit = eighth // 2
        while bit:
            for k, (before, level, at, place) in enumerate(seek):
                seen = jnp.take_along_axis(before, at + (bit - 1), axis=1, mode="promise_in_bounds")
                seek[k] = before, level, jnp.where(seen <= level, at + bit, at), place
            bit //= 2
        for k in range(n):
            _, _, at, place = seek[k]
            p, other = position(k)
            dx, dy, _ = shell[k]
            p += [rows(dx, dy, other, c) for c in range(3, 6)]
            for c in range(6):
                moved[k, c] = jnp.take_along_axis(p[c], at, axis=1, mode="promise_in_bounds")
            moved_keys[k] = jnp.take_along_axis(keys_of(dx, dy, other), at, axis=1, mode="promise_in_bounds")
            for block in range(2):
                here = place == block
                motion, key = ready[block]
                motion = [jnp.where(here, moved[k, c], motion[c]) for c in range(6)]
                ready[block] = motion, jnp.where(here, moved_keys[k], key)
        for block in range(2):
            keep(block, *ready[block])
        return start

    def keep(block, motion, key):
        for c in range(6):
            near[block, c] = motion[c]
        near[block, 6] = (key & 1).astype(jnp.float32)
        near_keys[block, 0] = key
        near_keys[block, 1] = key * KEY_B

    def assemble(block, carry):
        motion, key = empty()
        for k in range(n):
            here = places[k] == block
            motion = [jnp.where(here, moved[k, c], motion[c]) for c in range(6)]
            key = jnp.where(here, moved_keys[k], key)
        keep(block, motion, key)
        return carry

    def pair_blocks(tile, y, blocks, height, before):
        sides = []
        for block in blocks:
            other = [jnp.broadcast_to(near[block, c, pl.ds(y, 1), :], (8, slots)) for c in range(7)]
            key = jnp.broadcast_to(near_keys[block, 0, pl.ds(y, 1), :], (8, slots))
            offset = jnp.broadcast_to(near_keys[block, 1, pl.ds(y, 1), :], (8, slots))
            sides.append((other, key, offset, other[6] < 0.5))
        for g in range(0, height, 8):
            at = pl.ds(g, 8)
            own = [wide[tile, c, at, :] for c in range(8)]
            own_key, own_offset = wide_keys[tile, 0, at, :], wide_keys[tile, 1, at, :]
            total = [before[tile, c, at, :] for c in range(3)]
            for side in sides:
                terms = pair_strength(own, own_key, own_offset, own[6], own[7], *side)
                total = [a + b for a, b in zip(total, terms)]
            for c in range(3):
                forces[tile, c, at, :] = total[c]

    heights = list(range(slots // 2, slots + 1, STEP))

    def tile_pairs(zz, y, carry):
        tile = zz * out_y + y

        def at_height(height):
            def run():
                pair_blocks(tile, y, (0, 1), height, own_forces)

                def one(block, carry):
                    pair_blocks(tile, y, (block,), height, forces)
                    return carry

                lax.fori_loop(2, limits[0, tile], one, 0)

            return run

        lax.switch(limits[1, tile], [at_height(h) for h in heights])
        return carry

    ones = jnp.ones((2 * slots, slots), jnp.bfloat16)
    wide_lane = lax.broadcasted_iota(jnp.int32, (slots, slots), 1)
    for zz in range(out_z):
        z = gz * out_z + zz
        total = place_candidates(z)
        present = rows(0, 0, z, 0) < 0.5 * FAR
        blocks = jnp.maximum(1, (total.astype(jnp.int32) + (slots - 1)) >> lane_bits)
        count = jnp.sum(jnp.where(present, 1.0, 0.0), axis=1, keepdims=True).astype(jnp.int32)
        which = jnp.maximum((count + (STEP - 1)) // STEP - heights[0] // STEP, 0)
        for y in range(out_y):
            limits[0, zz * out_y + y] = blocks[y, 0]
            limits[1, zz * out_y + y] = which[y, 0]
        lax.fori_loop(2, jnp.max(blocks), assemble, 0)
        lax.fori_loop(0, out_y, functools.partial(tile_pairs, zz), 0)
        total = jnp.zeros((slots, slots), jnp.float32)
        for y in range(out_y):
            for c in range(3):
                whole = forces[zz * out_y + y, c]
                if c < 2:
                    sums = jnp.sum(whole, axis=1, keepdims=True)
                else:
                    high = whole.astype(jnp.bfloat16)
                    low = (whole - high.astype(jnp.float32)).astype(jnp.bfloat16)
                    sums = jnp.dot(jnp.concatenate([high, low], axis=1), ones, preferred_element_type=jnp.float32)
                total = jnp.where(wide_lane == c * out_y + y, sums, total)
        kicks = jnp.transpose(total)
        for c in range(3):
            kick = jnp.where(present, kick_scale * UNIT * kicks[c * out_y : (c + 1) * out_y], 0.0)
            for y in range(out_y):
                out_ref[c, 0, y, pl.ds(zz, 1), :] = kick[y : y + 1]


def on_device(nx, ny, nz, positions, velocities, bead_keys, counts):
    _, _, block_y, tiles_z, slots = positions.shape
    out_y, out_z = block_y * nz, tiles_z // nz
    span = out_y + 2
    tiles = out_y * out_z
    gathered = pl.pallas_call(
        functools.partial(gather_kernel, (nx, ny, nz, block_y, tiles_z)),
        out_shape=[
            jax.ShapeDtypeStruct((3, tiles_z, span, ROWS, slots), jnp.float32),
            jax.ShapeDtypeStruct((tiles, 8, slots, slots), jnp.float32),
            jax.ShapeDtypeStruct((tiles, 2, slots, slots), jnp.int32),
            jax.ShapeDtypeStruct((tiles, 3, slots, slots), jnp.float32),
            jax.ShapeDtypeStruct((slots, 9 * slots), jnp.bfloat16),
        ],
        in_specs=[pl.BlockSpec(memory_space=pltpu.HBM)] * 4,
        out_specs=[pl.BlockSpec(memory_space=pltpu.VMEM)] * 5,
        scratch_shapes=[
            pltpu.VMEM(positions.shape, jnp.float32),
            pltpu.VMEM(velocities.shape, jnp.float32),
            pltpu.VMEM(bead_keys.shape, jnp.int32),
            pltpu.SMEM((1, tiles_z, block_y), jnp.int32),
            pltpu.VMEM((tiles_z, block_y, ROWS, slots), jnp.float32),
            pltpu.VMEM((3 * ROWS, ROWS * slots), jnp.bfloat16),
            pltpu.SemaphoreType.DMA((3, nz)),
            pltpu.SemaphoreType.DMA((3, nz)),
            pltpu.SemaphoreType.DMA((2, 3, nz)),
            pltpu.SemaphoreType.DMA((2, 3)),
            pltpu.SemaphoreType.DMA,
            pltpu.SemaphoreType.DMA((4,)),
        ],
        compiler_params=pltpu.CompilerParams(
            collective_id=0, has_side_effects=True, vmem_limit_bytes=12582912
        ),
        name="gather_tiles",
    )(*(pltpu.with_memory_space_constraint(a, pltpu.HBM) for a in (positions, velocities, bead_keys, jnp.swapaxes(counts, 1, 2))))
    shells = len(shell_of(tiles_z))
    return pl.pallas_call(
        functools.partial(pair_kernel, (tiles_z, block_y, out_y, out_z)),
        out_shape=jax.ShapeDtypeStruct((3, 1, out_y, out_z, slots), jnp.float32),
        in_specs=[pl.BlockSpec(memory_space=pltpu.VMEM)] * 5,
        out_specs=pl.BlockSpec(memory_space=pltpu.VMEM),
        scratch_shapes=[
            pltpu.VMEM((shells * out_y, slots), jnp.float32),
            pltpu.VMEM((shells, out_y, slots), jnp.int32),
            pltpu.VMEM((shells, 6, out_y, slots), jnp.float32),
            pltpu.VMEM((shells, out_y, slots), jnp.int32),
            pltpu.VMEM((shells, 7, out_y, slots), jnp.float32),
            pltpu.VMEM((shells, 2, out_y, slots), jnp.int32),
            pltpu.VMEM((tiles, 3, slots, slots), jnp.float32),
            pltpu.SMEM((2, tiles), jnp.int32),
        ],
        compiler_params=pltpu.CompilerParams(vmem_limit_bytes=16777216),
        name="pair_kicks",
    )(*gathered)


def solution(mesh):
    in_specs = (
        P(None, "gx", ("gy", "gz"), None, None),
        P(None, "gx", ("gy", "gz"), None, None),
        P("gx", ("gy", "gz"), None, None),
        P("gx", ("gy", "gz"), None),
    )
    out_specs = P(None, "gx", "gy", "gz", None)
    nx, ny, nz = mesh.shape["gx"], mesh.shape["gy"], mesh.shape["gz"]
    return jax.shard_map(
        functools.partial(on_device, nx, ny, nz),
        mesh=mesh,
        in_specs=in_specs,
        out_specs=out_specs,
        check_vma=False,
    )
```

```python
import functools

import jax
import jax.numpy as jnp
from jax import lax
from jax.experimental import pallas as pl
from jax.experimental.pallas import tpu as pltpu
from jax.sharding import PartitionSpec as P

SIDE = 3.0

soft_radius = 0.05
friction = 4.5
noise_amplitude = 15.0
like_repulsion = 25.0
unlike_extra = 15.0
kick_scale = 0.02
root_twelve = 3.4641016151377544

FAR = 1.0e9
ROWS = 8
KEY_A = 1103515245
KEY_B = 12345
KEY_C = 747796405
STEP = 16
REACH = 1.00001
UNIT = noise_amplitude * root_twelve / 2147483648.0
MESH = pl.DeviceIdType.MESH


def pair_strength(own, own_key, own_offset, own_even, own_odd, other, key, offset, even):
    sep = [own[c] - other[c] for c in range(3)]
    squared = sep[0] * sep[0] + sep[1] * sep[1] + sep[2] * sep[2]
    root = lax.rsqrt(jnp.maximum(squared, 1e-30))
    scaled = jnp.maximum(1.0 - squared * root, 0.0) * jnp.minimum(root, 1.0 / soft_radius)
    dot = sep[0] * (own[3] - other[3]) + sep[1] * (own[4] - other[4]) + sep[2] * (own[5] - other[5])
    hashed = (own_key ^ key) * KEY_A + (own_offset + offset)
    hashed = hashed ^ lax.shift_right_logical(hashed, 15)
    hashed = hashed * KEY_C
    hashed = hashed ^ lax.shift_right_logical(hashed, 13)
    push = (hashed & 0x7FFFFF80).astype(jnp.float32) + jnp.where(even, own_even, own_odd)
    strength = scaled * (push - scaled * dot)
    return [strength * part for part in sep]


def split(values):
    high = values.astype(jnp.bfloat16).astype(jnp.float32)
    middle = (values - high).astype(jnp.bfloat16).astype(jnp.float32)
    return [high, middle, values - high - middle]


def column_of(tiles_z):
    return [None] if tiles_z == 2 else [-1, 1]


def own_tile(tile, brick, y, z, paired, select, wide, wide_keys, forces):
    tiles_z, block_y, _, slots = brick.shape
    rows = brick[z, y]
    parts = split(rows)
    spread = jnp.dot(jnp.transpose(jnp.concatenate(parts, axis=0)).astype(jnp.bfloat16), select[...], preferred_element_type=jnp.float32)

    def side(near, dz, shift_y=None):
        motion = [near[c : c + 1] for c in range(6)]
        if dz is None:
            motion[2] = motion[2] + jnp.where(motion[2] < 0.5 * SIDE, SIDE, -SIDE)
        elif dz:
            motion[2] = motion[2] + SIDE * dz
        if shift_y is not None:
            motion[1] = motion[1] + shift_y
        key = near[6:7].astype(jnp.int32) * 32768 + near[7:8].astype(jnp.int32)
        motion, key = [jnp.broadcast_to(m, (8, slots)) for m in motion], jnp.broadcast_to(key, (8, slots))
        return motion, key, key * KEY_B, (key & 1) == 0

    sides = [side(rows, 0)]
    for dz in column_of(tiles_z):
        sides.append(side(brick[1 - z if dz is None else lax.rem(z + dz + tiles_z, tiles_z), y], dz))
    if paired and block_y > 1:
        step = 1 - 2 * (y // (block_y // 2))
        sides.append(side(brick[z, y + step], 0, step.astype(jnp.float32) * SIDE))
    level = (like_repulsion - 0.5 * noise_amplitude * root_twelve) / UNIT
    for g in range(0, slots, 8):
        at = pl.ds(g, 8)
        part = [spread[g : g + 8, c * slots : (c + 1) * slots] for c in range(8)]
        low = part[7].astype(jnp.int32)
        own_key = part[6].astype(jnp.int32) * 32768 + low
        own_offset = own_key * KEY_B
        kind = (low & 1).astype(jnp.float32) * (unlike_extra / UNIT)
        own_even = level + kind
        own_odd = (level + unlike_extra / UNIT) - kind
        for c in range(6):
            wide[tile, c, at, :] = part[c]
        wide[tile, 6, at, :] = own_even
        wide[tile, 7, at, :] = own_odd
        wide_keys[tile, 0, at, :] = own_key
        wide_keys[tile, 1, at, :] = own_offset
        terms = [pair_strength(part, own_key, own_offset, own_even, own_odd, *one) for one in sides]
        for c in range(3):
            forces[tile, c, at, :] = functools.reduce(jnp.add, [term[c] for term in terms])


def gather_kernel(sizes, pos_in, vel_in, key_in, count_in, all_ref, wide, wide_keys, forces, below, pos_ref, vel_ref, key_ref, count_ref, packed, select, send, recv, edge_send, edge_recv, local, loads):
    nx, ny, nz, block_y, tiles_z = sizes
    gx, gy, gz = lax.axis_index("gx"), lax.axis_index("gy"), lax.axis_index("gz")
    slots = pos_ref.shape[-1]
    inputs = ((pos_in, pos_ref), (vel_in, vel_ref), (key_in, key_ref), (count_in, count_ref))
    fetches = [pltpu.make_async_copy(a, b, loads.at[k]) for k, (a, b) in enumerate(inputs)]
    for fetch in fetches:
        fetch.start()
    top = nz * block_y + 1
    barrier = pltpu.get_barrier_semaphore()

    def target(e, group, member):
        return (lax.rem(gx + e + nx, nx), lax.rem(gy + group + ny, ny), lax.rem(member + nz, nz))

    steps = (-1, 0, 1)
    for e in (-1, 1, 0):
        pl.semaphore_signal(barrier, inc=1, device_id=target(e, -1, nz - 1), device_id_type=MESH)
        pl.semaphore_signal(barrier, inc=1, device_id=target(e, 1, 0), device_id_type=MESH)
    for r in reversed(range(nz)):
        for e in (-1, 1, 0):
            if e or r:
                pl.semaphore_signal(barrier, inc=1, device_id=target(e, 0, gz + r), device_id_type=MESH)

    row = lax.broadcasted_iota(jnp.int32, select.shape, 0)
    column = lax.broadcasted_iota(jnp.int32, select.shape, 1)
    chosen = (row & (ROWS - 1)) == (column >> (slots - 1).bit_length())
    select[...] = jnp.where(chosen, 1.0, 0.0).astype(jnp.bfloat16)
    lane_bits = (slots - 1).bit_length()
    row = lax.broadcasted_iota(jnp.int32, below.shape, 0)
    column = lax.broadcasted_iota(jnp.int32, below.shape, 1)
    limit = jnp.where(column < slots, column + 1, (column >> lane_bits) * (slots // 8))
    below[...] = jnp.where(row < limit, 1.0, 0.0).astype(jnp.bfloat16)
    for fetch in fetches:
        fetch.wait()
    lane = lax.broadcasted_iota(jnp.int32, (1, slots), 1)
    for y in range(block_y):
        for z in range(tiles_z):
            present = lane < count_ref[0, z, y]
            key = key_ref[0, y, pl.ds(z, 1), :]
            rows = [jnp.where(present, pos_ref[c, 0, y, pl.ds(z, 1), :], FAR) for c in range(3)]
            rows += [vel_ref[c, 0, y, pl.ds(z, 1), :] * (friction / UNIT) for c in range(3)]
            rows += [(key >> 15).astype(jnp.float32), (key & 32767).astype(jnp.float32)]
            packed[z, y] = jnp.concatenate(rows, axis=0)

    def group_copy(e, r, slot_of):
        return pltpu.make_async_remote_copy(
            src_ref=packed,
            dst_ref=all_ref.at[1 - e, :, pl.ds(1 + slot_of * block_y, block_y)],
            send_sem=send.at[e + 1, r],
            recv_sem=recv.at[e + 1, r],
            device_id=target(e, 0, gz + r),
            device_id_type=MESH,
        )

    def edge_copy(e, side, member):
        first = side == 0
        return pltpu.make_async_remote_copy(
            src_ref=packed.at[:, pl.ds(0 if first else block_y - 1, 1)],
            dst_ref=all_ref.at[1 - e, :, pl.ds(top if first else 0, 1)],
            send_sem=edge_send.at[side, e + 1, member],
            recv_sem=edge_recv.at[side, e + 1],
            device_id=target(e, -1 if first else 1, member),
            device_id_type=MESH,
        )

    ends = jnp.where(gz == 0, 1, 0) + jnp.where(gz == nz - 1, 1, 0)
    pl.semaphore_wait(barrier, 3 * nz - 1 + 3 * nz * ends)

    def edges(side, act):
        for e in (-1, 1, 0):
            for member in range(nz):
                act(edge_copy(e, side, member))

    @pl.when(gz == 0)
    def _():
        edges(0, lambda c: c.start())

    @pl.when(gz == nz - 1)
    def _():
        edges(1, lambda c: c.start())

    for r in reversed(range(nz)):
        for e in (0, -1, 1):
            if e or r:
                group_copy(e, r, gz).start()

    mine = pltpu.make_async_copy(packed, all_ref.at[1, :, pl.ds(1 + gz * block_y, block_y)], local)
    mine.start()
    out_y, out_z = nz * block_y, tiles_z // nz
    for zz in range(out_z):

        def near_one(y, carry, zz=zz):
            own_tile(zz * out_y + gz * block_y + y, packed, y, gz * out_z + zz, True, select, wide, wide_keys, forces)
            return carry

        lax.fori_loop(0, block_y, near_one, 0, unroll=min(4, block_y))

    for r in range(1, nz):
        slot_of = lax.rem(gz - r + nz, nz)
        group_copy(0, r, slot_of).wait_recv()
        for zz in range(out_z):

            def remote(y, carry, zz=zz, slot_of=slot_of):
                at = slot_of * block_y + y
                own_tile(zz * out_y + at, all_ref.at[1, :, pl.ds(1 + slot_of * block_y, block_y)], y, gz * out_z + zz, False, select, wide, wide_keys, forces)
                return carry

            lax.fori_loop(0, block_y, remote, 0, unroll=min(4, block_y))

    mine.wait()
    for e in steps:
        for r in range(nz):
            if e or r:
                copy = group_copy(e, r, lax.rem(gz - r + nz, nz))
                if e:
                    copy.wait_recv()
                copy.wait_send()
        for side in range(2):
            edge_copy(e, side, 0).wait_recv()

    @pl.when(gz == 0)
    def _():
        edges(0, lambda c: c.wait_send())

    @pl.when(gz == nz - 1)
    def _():
        edges(1, lambda c: c.wait_send())


def shell_of(tiles_z):
    layers = (0, None) if tiles_z == 2 else (-1, 0, 1)
    offsets = [(dx, dy, dz) for dx in (-1, 0, 1) for dy in (-1, 0, 1) for dz in layers]
    done = [(0, 0, dz) for dz in [0] + column_of(tiles_z)]
    return [offset for offset in offsets if offset not in done]


def pair_kernel(sizes, all_ref, wide, wide_keys, own_forces, below, out_ref, masks, places, moved, moved_keys, near, near_keys, forces, limits):
    tiles_z, block_y, out_y, out_z = sizes
    slots = all_ref.shape[-1]
    span = all_ref.shape[2]
    gz = lax.axis_index("gz")
    shell = shell_of(tiles_z)
    n = len(shell)
    lane_bits = (slots - 1).bit_length()
    eighth = slots // 8
    flat = all_ref.reshape(3 * span * tiles_z * ROWS, slots)
    lane = lax.broadcasted_iota(jnp.int32, (out_y, slots), 1)
    line = lax.broadcasted_iota(jnp.int32, (out_y, slots), 0)

    def rows(dx, dy, z, c):
        start = (((1 + dx) * tiles_z + z) * span + 1 + dy) * ROWS + c
        return flat[pl.ds(start, out_y, stride=ROWS), :]

    def keys_of(dx, dy, z):
        return rows(dx, dy, z, 6).astype(jnp.int32) * 32768 + rows(dx, dy, z, 7).astype(jnp.int32)

    def empty():
        motion = [jnp.full((out_y, slots), FAR if c < 3 else 0.0, jnp.float32) for c in range(6)]
        return motion, jnp.zeros((out_y, slots), jnp.int32)

    def place_candidates(z):
        def position(k):
            dx, dy, dz = shell[k]
            other = 1 - z if dz is None else lax.rem(z + dz + tiles_z, tiles_z)
            p = [rows(dx, dy, other, c) for c in range(3)]
            if dx:
                p[0] = p[0] + SIDE * dx
            if dy:
                p[1] = p[1] + SIDE * dy
            if dz is None:
                p[2] = p[2] + jnp.where(p[2] < 0.5 * SIDE, SIDE, -SIDE)
            elif dz:
                p[2] = p[2] + SIDE * dz
            return p, other

        for k in range(n):
            dx, dy, dz = shell[k]
            other = 1 - z if dz is None else lax.rem(z + dz + tiles_z, tiles_z)
            gap = None
            for c, side in enumerate((dx, dy, dz)):
                if side != 0:
                    value = rows(dx, dy, other, c)
                    if side is None:
                        value = jnp.minimum(value, SIDE - value)
                    elif side < 0:
                        value = SIDE - value
                    gap = value * value if gap is None else gap + value * value
            inside = gap < REACH
            if dx == 0 and dz == 0 and block_y > 1:
                step = 1 - 2 * ((line % block_y) // (block_y // 2))
                inside = inside & ((step != dy) | (line < gz * block_y) | (line >= (gz + 1) * block_y))
            masks[pl.ds(k * out_y, out_y), :] = jnp.where(inside, 1.0, 0.0)

        sums = jnp.dot(masks[...].astype(jnp.bfloat16), below[...], preferred_element_type=jnp.float32)
        start = jnp.zeros((out_y, slots), jnp.float32)
        ready = [empty(), empty()]
        seek = []
        for k in range(n):
            part = [sums[k * out_y : (k + 1) * out_y, q * slots : (q + 1) * slots] for q in range(9)]
            first = start.astype(jnp.int32)
            want = (lane - first) & (slots - 1)
            level = want.astype(jnp.float32)
            upper = part[4] <= level
            second = jnp.where(upper, part[6], part[2]) <= level
            third = jnp.where(second, jnp.where(upper, part[7], part[3]), jnp.where(upper, part[5], part[1])) <= level
            at = jnp.where(upper, 4 * eighth, 0) + jnp.where(second, 2 * eighth, 0) + jnp.where(third, eighth, 0)
            place = jnp.where(level < part[8], (first + want) >> lane_bits, -1)
            places[k] = place
            seek.append((part[0], level, at, place))
            start = start + part[8]
        bit = eighth // 2
        while bit:
            for k, (before, level, at, place) in enumerate(seek):
                seen = jnp.take_along_axis(before, at + (bit - 1), axis=1, mode="promise_in_bounds")
                seek[k] = before, level, jnp.where(seen <= level, at + bit, at), place
            bit //= 2
        for k in range(n):
            _, _, at, place = seek[k]
            p, other = position(k)
            dx, dy, _ = shell[k]
            p += [rows(dx, dy, other, c) for c in range(3, 6)]
            for c in range(6):
                moved[k, c] = jnp.take_along_axis(p[c], at, axis=1, mode="promise_in_bounds")
            moved_keys[k] = jnp.take_along_axis(keys_of(dx, dy, other), at, axis=1, mode="promise_in_bounds")
            for block in range(2):
                here = place == block
                motion, key = ready[block]
                motion = [jnp.where(here, moved[k, c], motion[c]) for c in range(6)]
                ready[block] = motion, jnp.where(here, moved_keys[k], key)
        for block in range(2):
            keep(block, *ready[block])
        return start

    def keep(block, motion, key):
        for c in range(6):
            near[block, c] = motion[c]
        near[block, 6] = (key & 1).astype(jnp.float32)
        near_keys[block, 0] = key
        near_keys[block, 1] = key * KEY_B

    def assemble(block, carry):
        motion, key = empty()
        for k in range(n):
            here = places[k] == block
            motion = [jnp.where(here, moved[k, c], motion[c]) for c in range(6)]
            key = jnp.where(here, moved_keys[k], key)
        keep(block, motion, key)
        return carry

    def pair_blocks(tile, y, blocks, height, before):
        sides = []
        for block in blocks:
            other = [jnp.broadcast_to(near[block, c, pl.ds(y, 1), :], (8, slots)) for c in range(7)]
            key = jnp.broadcast_to(near_keys[block, 0, pl.ds(y, 1), :], (8, slots))
            offset = jnp.broadcast_to(near_keys[block, 1, pl.ds(y, 1), :], (8, slots))
            sides.append((other, key, offset, other[6] < 0.5))
        for g in range(0, height, 8):
            at = pl.ds(g, 8)
            own = [wide[tile, c, at, :] for c in range(8)]
            own_key, own_offset = wide_keys[tile, 0, at, :], wide_keys[tile, 1, at, :]
            total = [before[tile, c, at, :] for c in range(3)]
            for side in sides:
                terms = pair_strength(own, own_key, own_offset, own[6], own[7], *side)
                total = [a + b for a, b in zip(total, terms)]
            for c in range(3):
                forces[tile, c, at, :] = total[c]

    heights = list(range(slots // 2, slots + 1, STEP))

    def tile_pairs(zz, y, carry):
        tile = zz * out_y + y

        def at_height(height):
            def run():
                pair_blocks(tile, y, (0, 1), height, own_forces)

                def one(block, carry):
                    pair_blocks(tile, y, (block,), height, forces)
                    return carry

                lax.fori_loop(2, limits[0, tile], one, 0)

            return run

        lax.switch(limits[1, tile], [at_height(h) for h in heights])
        return carry

    ones = jnp.ones((2 * slots, slots), jnp.bfloat16)
    wide_lane = lax.broadcasted_iota(jnp.int32, (slots, slots), 1)
    for zz in range(out_z):
        z = gz * out_z + zz
        total = place_candidates(z)
        present = rows(0, 0, z, 0) < 0.5 * FAR
        blocks = jnp.maximum(1, (total.astype(jnp.int32) + (slots - 1)) >> lane_bits)
        count = jnp.sum(jnp.where(present, 1.0, 0.0), axis=1, keepdims=True).astype(jnp.int32)
        which = jnp.maximum((count + (STEP - 1)) // STEP - heights[0] // STEP, 0)
        for y in range(out_y):
            limits[0, zz * out_y + y] = blocks[y, 0]
            limits[1, zz * out_y + y] = which[y, 0]
        lax.fori_loop(2, jnp.max(blocks), assemble, 0)
        lax.fori_loop(0, out_y, functools.partial(tile_pairs, zz), 0)
        total = jnp.zeros((slots, slots), jnp.float32)
        for y in range(out_y):
            for c in range(3):
                whole = forces[zz * out_y + y, c]
                if c < 2:
                    sums = jnp.sum(whole, axis=1, keepdims=True)
                else:
                    high = whole.astype(jnp.bfloat16)
                    low = (whole - high.astype(jnp.float32)).astype(jnp.bfloat16)
                    sums = jnp.dot(jnp.concatenate([high, low], axis=1), ones, preferred_element_type=jnp.float32)
                total = jnp.where(wide_lane == c * out_y + y, sums, total)
        kicks = jnp.transpose(total)
        for c in range(3):
            kick = jnp.where(present, kick_scale * UNIT * kicks[c * out_y : (c + 1) * out_y], 0.0)
            for y in range(out_y):
                out_ref[c, 0, y, pl.ds(zz, 1), :] = kick[y : y + 1]


def on_device(nx, ny, nz, positions, velocities, bead_keys, counts):
    _, _, block_y, tiles_z, slots = positions.shape
    out_y, out_z = block_y * nz, tiles_z // nz
    span = out_y + 2
    tiles = out_y * out_z
    gathered = pl.pallas_call(
        functools.partial(gather_kernel, (nx, ny, nz, block_y, tiles_z)),
        out_shape=[
            jax.ShapeDtypeStruct((3, tiles_z, span, ROWS, slots), jnp.float32),
            jax.ShapeDtypeStruct((tiles, 8, slots, slots), jnp.float32),
            jax.ShapeDtypeStruct((tiles, 2, slots, slots), jnp.int32),
            jax.ShapeDtypeStruct((tiles, 3, slots, slots), jnp.float32),
            jax.ShapeDtypeStruct((slots, 9 * slots), jnp.bfloat16),
        ],
        in_specs=[pl.BlockSpec(memory_space=pltpu.HBM)] * 4,
        out_specs=[pl.BlockSpec(memory_space=pltpu.VMEM)] * 5,
        scratch_shapes=[
            pltpu.VMEM(positions.shape, jnp.float32),
            pltpu.VMEM(velocities.shape, jnp.float32),
            pltpu.VMEM(bead_keys.shape, jnp.int32),
            pltpu.SMEM((1, tiles_z, block_y), jnp.int32),
            pltpu.VMEM((tiles_z, block_y, ROWS, slots), jnp.float32),
            pltpu.VMEM((3 * ROWS, ROWS * slots), jnp.bfloat16),
            pltpu.SemaphoreType.DMA((3, nz)),
            pltpu.SemaphoreType.DMA((3, nz)),
            pltpu.SemaphoreType.DMA((2, 3, nz)),
            pltpu.SemaphoreType.DMA((2, 3)),
            pltpu.SemaphoreType.DMA,
            pltpu.SemaphoreType.DMA((4,)),
        ],
        compiler_params=pltpu.CompilerParams(
            collective_id=0, has_side_effects=True, vmem_limit_bytes=12582912
        ),
        name="gather_tiles",
    )(*(pltpu.with_memory_space_constraint(a, pltpu.HBM) for a in (positions, velocities, bead_keys, jnp.swapaxes(counts, 1, 2))))
    shells = len(shell_of(tiles_z))
    return pl.pallas_call(
        functools.partial(pair_kernel, (tiles_z, block_y, out_y, out_z)),
        out_shape=jax.ShapeDtypeStruct((3, 1, out_y, out_z, slots), jnp.float32),
        in_specs=[pl.BlockSpec(memory_space=pltpu.VMEM)] * 5,
        out_specs=pl.BlockSpec(memory_space=pltpu.VMEM),
        scratch_shapes=[
            pltpu.VMEM((shells * out_y, slots), jnp.float32),
            pltpu.VMEM((shells, out_y, slots), jnp.int32),
            pltpu.VMEM((shells, 6, out_y, slots), jnp.float32),
            pltpu.VMEM((shells, out_y, slots), jnp.int32),
            pltpu.VMEM((shells, 7, out_y, slots), jnp.float32),
            pltpu.VMEM((shells, 2, out_y, slots), jnp.int32),
            pltpu.VMEM((tiles, 3, slots, slots), jnp.float32),
            pltpu.SMEM((2, tiles), jnp.int32),
        ],
        compiler_params=pltpu.CompilerParams(vmem_limit_bytes=16777216),
        name="pair_kicks",
    )(*gathered)


def solution(mesh):
    in_specs = (
        P(None, "gx", ("gy", "gz"), None, None),
        P(None, "gx", ("gy", "gz"), None, None),
        P("gx", ("gy", "gz"), None, None),
        P("gx", ("gy", "gz"), None),
    )
    out_specs = P(None, "gx", "gy", "gz", None)
    nx, ny, nz = mesh.shape["gx"], mesh.shape["gy"], mesh.shape["gz"]
    return jax.shard_map(
        functools.partial(on_device, nx, ny, nz),
        mesh=mesh,
        in_specs=in_specs,
        out_specs=out_specs,
        check_vma=False,
    )
```

```python
import functools

import jax
import jax.numpy as jnp
from jax import lax
from jax.experimental import pallas as pl
from jax.experimental.pallas import tpu as pltpu
from jax.sharding import PartitionSpec as P

SIDE = 3.0

soft_radius = 0.05
friction = 4.5
noise_amplitude = 15.0
like_repulsion = 25.0
unlike_extra = 15.0
kick_scale = 0.02
root_twelve = 3.4641016151377544

FAR = 1.0e9
ROWS = 8
KEY_A = 1103515245
KEY_B = 12345
KEY_C = 747796405
STEP = 16
REACH = 1.00001
UNIT = noise_amplitude * root_twelve / 2147483648.0
MESH = pl.DeviceIdType.MESH


def pair_strength(own, own_key, own_offset, own_even, own_odd, other, key, offset, even):
    sep = [own[c] - other[c] for c in range(3)]
    squared = sep[0] * sep[0] + sep[1] * sep[1] + sep[2] * sep[2]
    root = lax.rsqrt(jnp.maximum(squared, 1e-30))
    scaled = jnp.maximum(1.0 - squared * root, 0.0) * jnp.minimum(root, 1.0 / soft_radius)
    dot = sep[0] * (own[3] - other[3]) + sep[1] * (own[4] - other[4]) + sep[2] * (own[5] - other[5])
    hashed = (own_key ^ key) * KEY_A + (own_offset + offset)
    hashed = hashed ^ lax.shift_right_logical(hashed, 15)
    hashed = hashed * KEY_C
    hashed = hashed ^ lax.shift_right_logical(hashed, 13)
    push = (hashed & 0x7FFFFF80).astype(jnp.float32) + jnp.where(even, own_even, own_odd)
    strength = scaled * (push - scaled * dot)
    return [strength * part for part in sep]


def split(values):
    high = values.astype(jnp.bfloat16).astype(jnp.float32)
    middle = (values - high).astype(jnp.bfloat16).astype(jnp.float32)
    return [high, middle, values - high - middle]


def column_of(tiles_z):
    return [None] if tiles_z == 2 else [-1, 1]


def own_tile(tile, brick, y, z, paired, select, wide, wide_keys, forces):
    tiles_z, block_y, _, slots = brick.shape
    rows = brick[z, y]
    parts = split(rows)
    spread = jnp.dot(jnp.transpose(jnp.concatenate(parts, axis=0)).astype(jnp.bfloat16), select[...], preferred_element_type=jnp.float32)

    def side(near, dz, shift_y=None):
        motion = [near[c : c + 1] for c in range(6)]
        if dz is None:
            motion[2] = motion[2] + jnp.where(motion[2] < 0.5 * SIDE, SIDE, -SIDE)
        elif dz:
            motion[2] = motion[2] + SIDE * dz
        if shift_y is not None:
            motion[1] = motion[1] + shift_y
        key = near[6:7].astype(jnp.int32) * 32768 + near[7:8].astype(jnp.int32)
        motion, key = [jnp.broadcast_to(m, (8, slots)) for m in motion], jnp.broadcast_to(key, (8, slots))
        return motion, key, key * KEY_B, (key & 1) == 0

    sides = [side(rows, 0)]
    for dz in column_of(tiles_z):
        sides.append(side(brick[1 - z if dz is None else lax.rem(z + dz + tiles_z, tiles_z), y], dz))
    if paired and block_y > 1:
        step = 1 - 2 * (y // (block_y // 2))
        sides.append(side(brick[z, y + step], 0, step.astype(jnp.float32) * SIDE))
    level = (like_repulsion - 0.5 * noise_amplitude * root_twelve) / UNIT
    for g in range(0, slots, 8):
        at = pl.ds(g, 8)
        part = [spread[g : g + 8, c * slots : (c + 1) * slots] for c in range(8)]
        low = part[7].astype(jnp.int32)
        own_key = part[6].astype(jnp.int32) * 32768 + low
        own_offset = own_key * KEY_B
        kind = (low & 1).astype(jnp.float32) * (unlike_extra / UNIT)
        own_even = level + kind
        own_odd = (level + unlike_extra / UNIT) - kind
        for c in range(6):
            wide[tile, c, at, :] = part[c]
        wide[tile, 6, at, :] = own_even
        wide[tile, 7, at, :] = own_odd
        wide_keys[tile, 0, at, :] = own_key
        wide_keys[tile, 1, at, :] = own_offset
        terms = [pair_strength(part, own_key, own_offset, own_even, own_odd, *one) for one in sides]
        for c in range(3):
            forces[tile, c, at, :] = functools.reduce(jnp.add, [term[c] for term in terms])


def gather_kernel(sizes, pos_in, vel_in, key_in, count_in, all_ref, wide, wide_keys, forces, below, pos_ref, vel_ref, key_ref, count_ref, packed, select, send, recv, edge_send, edge_recv, local, loads):
    nx, ny, nz, block_y, tiles_z = sizes
    gx, gy, gz = lax.axis_index("gx"), lax.axis_index("gy"), lax.axis_index("gz")
    slots = pos_ref.shape[-1]
    inputs = ((pos_in, pos_ref), (vel_in, vel_ref), (key_in, key_ref), (count_in, count_ref))
    fetches = [pltpu.make_async_copy(a, b, loads.at[k]) for k, (a, b) in enumerate(inputs)]
    for fetch in fetches:
        fetch.start()
    top = nz * block_y + 1
    barrier = pltpu.get_barrier_semaphore()

    def target(e, group, member):
        return (lax.rem(gx + e + nx, nx), lax.rem(gy + group + ny, ny), lax.rem(member + nz, nz))

    steps = (-1, 0, 1)
    for e in (-1, 1, 0):
        pl.semaphore_signal(barrier, inc=1, device_id=target(e, -1, nz - 1), device_id_type=MESH)
        pl.semaphore_signal(barrier, inc=1, device_id=target(e, 1, 0), device_id_type=MESH)
    for r in reversed(range(nz)):
        for e in (-1, 1, 0):
            if e or r:
                pl.semaphore_signal(barrier, inc=1, device_id=target(e, 0, gz + r), device_id_type=MESH)

    row = lax.broadcasted_iota(jnp.int32, select.shape, 0)
    column = lax.broadcasted_iota(jnp.int32, select.shape, 1)
    chosen = (row & (ROWS - 1)) == (column >> (slots - 1).bit_length())
    select[...] = jnp.where(chosen, 1.0, 0.0).astype(jnp.bfloat16)
    lane_bits = (slots - 1).bit_length()
    row = lax.broadcasted_iota(jnp.int32, below.shape, 0)
    column = lax.broadcasted_iota(jnp.int32, below.shape, 1)
    limit = jnp.where(column < slots, column + 1, (column >> lane_bits) * (slots // 8))
    below[...] = jnp.where(row < limit, 1.0, 0.0).astype(jnp.bfloat16)
    for fetch in fetches:
        fetch.wait()
    lane = lax.broadcasted_iota(jnp.int32, (1, slots), 1)
    for y in range(block_y):
        for z in range(tiles_z):
            present = lane < count_ref[0, z, y]
            key = key_ref[0, y, pl.ds(z, 1), :]
            rows = [jnp.where(present, pos_ref[c, 0, y, pl.ds(z, 1), :], FAR) for c in range(3)]
            rows += [vel_ref[c, 0, y, pl.ds(z, 1), :] * (friction / UNIT) for c in range(3)]
            rows += [(key >> 15).astype(jnp.float32), (key & 32767).astype(jnp.float32)]
            packed[z, y] = jnp.concatenate(rows, axis=0)

    def group_copy(e, r, slot_of):
        return pltpu.make_async_remote_copy(
            src_ref=packed,
            dst_ref=all_ref.at[1 - e, :, pl.ds(1 + slot_of * block_y, block_y)],
            send_sem=send.at[e + 1, r],
            recv_sem=recv.at[e + 1, r],
            device_id=target(e, 0, gz + r),
            device_id_type=MESH,
        )

    def edge_copy(e, side, member):
        first = side == 0
        return pltpu.make_async_remote_copy(
            src_ref=packed.at[:, pl.ds(0 if first else block_y - 1, 1)],
            dst_ref=all_ref.at[1 - e, :, pl.ds(top if first else 0, 1)],
            send_sem=edge_send.at[side, e + 1, member],
            recv_sem=edge_recv.at[side, e + 1],
            device_id=target(e, -1 if first else 1, member),
            device_id_type=MESH,
        )

    ends = jnp.where(gz == 0, 1, 0) + jnp.where(gz == nz - 1, 1, 0)
    pl.semaphore_wait(barrier, 3 * nz - 1 + 3 * nz * ends)

    def edges(side, act):
        for e in (-1, 1, 0):
            for member in range(nz):
                act(edge_copy(e, side, member))

    @pl.when(gz == 0)
    def _():
        edges(0, lambda c: c.start())

    @pl.when(gz == nz - 1)
    def _():
        edges(1, lambda c: c.start())

    for r in reversed(range(nz)):
        for e in (0, -1, 1):
            if e or r:
                group_copy(e, r, gz).start()

    mine = pltpu.make_async_copy(packed, all_ref.at[1, :, pl.ds(1 + gz * block_y, block_y)], local)
    mine.start()
    out_y, out_z = nz * block_y, tiles_z // nz
    for zz in range(out_z):

        def near_one(y, carry, zz=zz):
            own_tile(zz * out_y + gz * block_y + y, packed, y, gz * out_z + zz, True, select, wide, wide_keys, forces)
            return carry

        lax.fori_loop(0, block_y, near_one, 0, unroll=min(4, block_y))

    for r in range(1, nz):
        slot_of = lax.rem(gz - r + nz, nz)
        group_copy(0, r, slot_of).wait_recv()
        for zz in range(out_z):

            def remote(y, carry, zz=zz, slot_of=slot_of):
                at = slot_of * block_y + y
                own_tile(zz * out_y + at, all_ref.at[1, :, pl.ds(1 + slot_of * block_y, block_y)], y, gz * out_z + zz, False, select, wide, wide_keys, forces)
                return carry

            lax.fori_loop(0, block_y, remote, 0, unroll=min(4, block_y))

    mine.wait()
    for e in steps:
        for r in range(nz):
            if e or r:
                copy = group_copy(e, r, lax.rem(gz - r + nz, nz))
                if e:
                    copy.wait_recv()
                copy.wait_send()
        for side in range(2):
            edge_copy(e, side, 0).wait_recv()

    @pl.when(gz == 0)
    def _():
        edges(0, lambda c: c.wait_send())

    @pl.when(gz == nz - 1)
    def _():
        edges(1, lambda c: c.wait_send())


def shell_of(tiles_z):
    layers = (0, None) if tiles_z == 2 else (-1, 0, 1)
    offsets = [(dx, dy, dz) for dx in (-1, 0, 1) for dy in (-1, 0, 1) for dz in layers]
    done = [(0, 0, dz) for dz in [0] + column_of(tiles_z)]
    return [offset for offset in offsets if offset not in done]


def pair_kernel(sizes, all_ref, wide, wide_keys, own_forces, below, out_ref, masks, places, moved, moved_keys, near, near_keys, forces, limits):
    tiles_z, block_y, out_y, out_z = sizes
    slots = all_ref.shape[-1]
    span = all_ref.shape[2]
    gz = lax.axis_index("gz")
    shell = shell_of(tiles_z)
    n = len(shell)
    lane_bits = (slots - 1).bit_length()
    eighth = slots // 8
    flat = all_ref.reshape(3 * span * tiles_z * ROWS, slots)
    lane = lax.broadcasted_iota(jnp.int32, (out_y, slots), 1)
    line = lax.broadcasted_iota(jnp.int32, (out_y, slots), 0)

    def rows(dx, dy, z, c):
        start = (((1 + dx) * tiles_z + z) * span + 1 + dy) * ROWS + c
        return flat[pl.ds(start, out_y, stride=ROWS), :]

    def keys_of(dx, dy, z):
        return rows(dx, dy, z, 6).astype(jnp.int32) * 32768 + rows(dx, dy, z, 7).astype(jnp.int32)

    def empty():
        motion = [jnp.full((out_y, slots), FAR if c < 3 else 0.0, jnp.float32) for c in range(6)]
        return motion, jnp.zeros((out_y, slots), jnp.int32)

    def place_candidates(z):
        def position(k):
            dx, dy, dz = shell[k]
            other = 1 - z if dz is None else lax.rem(z + dz + tiles_z, tiles_z)
            p = [rows(dx, dy, other, c) for c in range(3)]
            if dx:
                p[0] = p[0] + SIDE * dx
            if dy:
                p[1] = p[1] + SIDE * dy
            if dz is None:
                p[2] = p[2] + jnp.where(p[2] < 0.5 * SIDE, SIDE, -SIDE)
            elif dz:
                p[2] = p[2] + SIDE * dz
            return p, other

        for k in range(n):
            dx, dy, dz = shell[k]
            other = 1 - z if dz is None else lax.rem(z + dz + tiles_z, tiles_z)
            gap = None
            for c, side in enumerate((dx, dy, dz)):
                if side != 0:
                    value = rows(dx, dy, other, c)
                    if side is None:
                        value = jnp.minimum(value, SIDE - value)
                    elif side < 0:
                        value = SIDE - value
                    gap = value * value if gap is None else gap + value * value
            inside = gap < REACH
            if dx == 0 and dz == 0 and block_y > 1:
                step = 1 - 2 * ((line % block_y) // (block_y // 2))
                inside = inside & ((step != dy) | (line < gz * block_y) | (line >= (gz + 1) * block_y))
            masks[pl.ds(k * out_y, out_y), :] = jnp.where(inside, 1.0, 0.0)

        sums = jnp.dot(masks[...].astype(jnp.bfloat16), below[...], preferred_element_type=jnp.float32)
        start = jnp.zeros((out_y, slots), jnp.float32)
        ready = [empty(), empty()]
        seek = []
        for k in range(n):
            part = [sums[k * out_y : (k + 1) * out_y, q * slots : (q + 1) * slots] for q in range(9)]
            first = start.astype(jnp.int32)
            want = (lane - first) & (slots - 1)
            level = want.astype(jnp.float32)
            upper = part[4] <= level
            second = jnp.where(upper, part[6], part[2]) <= level
            third = jnp.where(second, jnp.where(upper, part[7], part[3]), jnp.where(upper, part[5], part[1])) <= level
            at = jnp.where(upper, 4 * eighth, 0) + jnp.where(second, 2 * eighth, 0) + jnp.where(third, eighth, 0)
            place = jnp.where(level < part[8], (first + want) >> lane_bits, -1)
            places[k] = place
            seek.append((part[0], level, at, place))
            start = start + part[8]
        bit = eighth // 2
        while bit:
            for k, (before, level, at, place) in enumerate(seek):
                seen = jnp.take_along_axis(before, at + (bit - 1), axis=1, mode="promise_in_bounds")
                seek[k] = before, level, jnp.where(seen <= level, at + bit, at), place
            bit //= 2
        for k in range(n):
            _, _, at, place = seek[k]
            p, other = position(k)
            dx, dy, _ = shell[k]
            p += [rows(dx, dy, other, c) for c in range(3, 6)]
            for c in range(6):
                moved[k, c] = jnp.take_along_axis(p[c], at, axis=1, mode="promise_in_bounds")
            moved_keys[k] = jnp.take_along_axis(keys_of(dx, dy, other), at, axis=1, mode="promise_in_bounds")
            for block in range(2):
                here = place == block
                motion, key = ready[block]
                motion = [jnp.where(here, moved[k, c], motion[c]) for c in range(6)]
                ready[block] = motion, jnp.where(here, moved_keys[k], key)
        for block in range(2):
            keep(block, *ready[block])
        return start

    def keep(block, motion, key):
        for c in range(6):
            near[block, c] = motion[c]
        near[block, 6] = (key & 1).astype(jnp.float32)
        near_keys[block, 0] = key
        near_keys[block, 1] = key * KEY_B

    def assemble(block, carry):
        motion, key = empty()
        for k in range(n):
            here = places[k] == block
            motion = [jnp.where(here, moved[k, c], motion[c]) for c in range(6)]
            key = jnp.where(here, moved_keys[k], key)
        keep(block, motion, key)
        return carry

    def pair_blocks(tile, y, blocks, height, before):
        sides = []
        for block in blocks:
            other = [jnp.broadcast_to(near[block, c, pl.ds(y, 1), :], (8, slots)) for c in range(7)]
            key = jnp.broadcast_to(near_keys[block, 0, pl.ds(y, 1), :], (8, slots))
            offset = jnp.broadcast_to(near_keys[block, 1, pl.ds(y, 1), :], (8, slots))
            sides.append((other, key, offset, other[6] < 0.5))
        for g in range(0, height, 8):
            at = pl.ds(g, 8)
            own = [wide[tile, c, at, :] for c in range(8)]
            own_key, own_offset = wide_keys[tile, 0, at, :], wide_keys[tile, 1, at, :]
            total = [before[tile, c, at, :] for c in range(3)]
            for side in sides:
                terms = pair_strength(own, own_key, own_offset, own[6], own[7], *side)
                total = [a + b for a, b in zip(total, terms)]
            for c in range(3):
                forces[tile, c, at, :] = total[c]

    heights = list(range(slots // 2, slots + 1, STEP))

    def tile_pairs(zz, y, carry):
        tile = zz * out_y + y

        def at_height(height):
            def run():
                pair_blocks(tile, y, (0, 1), height, own_forces)

                def one(block, carry):
                    pair_blocks(tile, y, (block,), height, forces)
                    return carry

                lax.fori_loop(2, limits[0, tile], one, 0)

            return run

        lax.switch(limits[1, tile], [at_height(h) for h in heights])
        return carry

    ones = jnp.ones((2 * slots, slots), jnp.bfloat16)
    wide_lane = lax.broadcasted_iota(jnp.int32, (slots, slots), 1)
    for zz in range(out_z):
        z = gz * out_z + zz
        total = place_candidates(z)
        present = rows(0, 0, z, 0) < 0.5 * FAR
        blocks = jnp.maximum(1, (total.astype(jnp.int32) + (slots - 1)) >> lane_bits)
        count = jnp.sum(jnp.where(present, 1.0, 0.0), axis=1, keepdims=True).astype(jnp.int32)
        which = jnp.maximum((count + (STEP - 1)) // STEP - heights[0] // STEP, 0)
        for y in range(out_y):
            limits[0, zz * out_y + y] = blocks[y, 0]
            limits[1, zz * out_y + y] = which[y, 0]
        lax.fori_loop(2, jnp.max(blocks), assemble, 0)
        lax.fori_loop(0, out_y, functools.partial(tile_pairs, zz), 0)
        total = jnp.zeros((slots, slots), jnp.float32)
        for y in range(out_y):
            for c in range(3):
                whole = forces[zz * out_y + y, c]
                if c + y % 2 < 2:
                    sums = jnp.sum(whole, axis=1, keepdims=True)
                else:
                    high = whole.astype(jnp.bfloat16)
                    low = (whole - high.astype(jnp.float32)).astype(jnp.bfloat16)
                    sums = jnp.dot(jnp.concatenate([high, low], axis=1), ones, preferred_element_type=jnp.float32)
                total = jnp.where(wide_lane == c * out_y + y, sums, total)
        kicks = jnp.transpose(total)
        for c in range(3):
            kick = jnp.where(present, kick_scale * UNIT * kicks[c * out_y : (c + 1) * out_y], 0.0)
            for y in range(out_y):
                out_ref[c, 0, y, pl.ds(zz, 1), :] = kick[y : y + 1]


def on_device(nx, ny, nz, positions, velocities, bead_keys, counts):
    _, _, block_y, tiles_z, slots = positions.shape
    out_y, out_z = block_y * nz, tiles_z // nz
    span = out_y + 2
    tiles = out_y * out_z
    gathered = pl.pallas_call(
        functools.partial(gather_kernel, (nx, ny, nz, block_y, tiles_z)),
        out_shape=[
            jax.ShapeDtypeStruct((3, tiles_z, span, ROWS, slots), jnp.float32),
            jax.ShapeDtypeStruct((tiles, 8, slots, slots), jnp.float32),
            jax.ShapeDtypeStruct((tiles, 2, slots, slots), jnp.int32),
            jax.ShapeDtypeStruct((tiles, 3, slots, slots), jnp.float32),
            jax.ShapeDtypeStruct((slots, 9 * slots), jnp.bfloat16),
        ],
        in_specs=[pl.BlockSpec(memory_space=pltpu.HBM)] * 4,
        out_specs=[pl.BlockSpec(memory_space=pltpu.VMEM)] * 5,
        scratch_shapes=[
            pltpu.VMEM(positions.shape, jnp.float32),
            pltpu.VMEM(velocities.shape, jnp.float32),
            pltpu.VMEM(bead_keys.shape, jnp.int32),
            pltpu.SMEM((1, tiles_z, block_y), jnp.int32),
            pltpu.VMEM((tiles_z, block_y, ROWS, slots), jnp.float32),
            pltpu.VMEM((3 * ROWS, ROWS * slots), jnp.bfloat16),
            pltpu.SemaphoreType.DMA((3, nz)),
            pltpu.SemaphoreType.DMA((3, nz)),
            pltpu.SemaphoreType.DMA((2, 3, nz)),
            pltpu.SemaphoreType.DMA((2, 3)),
            pltpu.SemaphoreType.DMA,
            pltpu.SemaphoreType.DMA((4,)),
        ],
        compiler_params=pltpu.CompilerParams(
            collective_id=0, has_side_effects=True, vmem_limit_bytes=12582912
        ),
        name="gather_tiles",
    )(*(pltpu.with_memory_space_constraint(a, pltpu.HBM) for a in (positions, velocities, bead_keys, jnp.swapaxes(counts, 1, 2))))
    shells = len(shell_of(tiles_z))
    return pl.pallas_call(
        functools.partial(pair_kernel, (tiles_z, block_y, out_y, out_z)),
        out_shape=jax.ShapeDtypeStruct((3, 1, out_y, out_z, slots), jnp.float32),
        in_specs=[pl.BlockSpec(memory_space=pltpu.VMEM)] * 5,
        out_specs=pl.BlockSpec(memory_space=pltpu.VMEM),
        scratch_shapes=[
            pltpu.VMEM((shells * out_y, slots), jnp.float32),
            pltpu.VMEM((shells, out_y, slots), jnp.int32),
            pltpu.VMEM((shells, 6, out_y, slots), jnp.float32),
            pltpu.VMEM((shells, out_y, slots), jnp.int32),
            pltpu.VMEM((shells, 7, out_y, slots), jnp.float32),
            pltpu.VMEM((shells, 2, out_y, slots), jnp.int32),
            pltpu.VMEM((tiles, 3, slots, slots), jnp.float32),
            pltpu.SMEM((2, tiles), jnp.int32),
        ],
        compiler_params=pltpu.CompilerParams(vmem_limit_bytes=16777216),
        name="pair_kicks",
    )(*gathered)


def solution(mesh):
    in_specs = (
        P(None, "gx", ("gy", "gz"), None, None),
        P(None, "gx", ("gy", "gz"), None, None),
        P("gx", ("gy", "gz"), None, None),
        P("gx", ("gy", "gz"), None),
    )
    out_specs = P(None, "gx", "gy", "gz", None)
    nx, ny, nz = mesh.shape["gx"], mesh.shape["gy"], mesh.shape["gz"]
    return jax.shard_map(
        functools.partial(on_device, nx, ny, nz),
        mesh=mesh,
        in_specs=in_specs,
        out_specs=out_specs,
        check_vma=False,
    )
```
